8 devices in a mesh: dp: 1 (over z), ep: 8 (over x, y, core).
Axes of the slice: x: 2, y: 2, z: 1, core: 2. Of those that a mesh axis runs over, the one named last changes fastest.
Arguments:
- x: bfloat16 [1, 8, 256, 3584], P('dp', 'ep')
- expert: int32 [1, 8, 256, 2], P('dp', 'ep')
- slot: int32 [1, 8, 256, 2], P('dp', 'ep')
- gate: float32 [1, 8, 256, 2], P('dp', 'ep')
- w_gate: bfloat16 [16, 3584, 4864], P('ep')
- w_up: bfloat16 [16, 3584, 4864], P('ep')
- w_down: bfloat16 [16, 4864, 3584], P('ep')
Outputs:
- y: bfloat16 [1, 8, 256, 3584], P('dp', 'ep')
All inputs are finite; a program needn't handle non-finite values.
Results may differ from the reference program's by a relative error of at most 0.009.
Values are sent between devices in bfloat16 or wider.
A program may use at most 2 GiB of HBM per device.

```python
import jax
import jax.numpy as jnp

MEMBERS = 8
TOKENS = 256
D = 3584
FF = 4864
TOP = 2
EXPERTS = 16
SLOTS = 5 * TOKENS * TOP // (4 * EXPERTS)


def setup_inputs(seed: int = 0, part: int = 0) -> dict:
    own, k1, k2, k3, k4, k5, k6 = jax.random.split(jax.random.key(seed), 7)
    kx, ke, kl, kg = jax.random.split(jax.random.fold_in(own, part), 4)
    devices = (1, MEMBERS)
    place = jax.random.permutation(kl, jnp.arange(EXPERTS, dtype=jnp.uint32))
    slow = ((EXPERTS + (9 * place) % EXPERTS) << ((9 * place) // EXPERTS)) // EXPERTS
    wait = (jax.random.bits(ke, (*devices, TOKENS, EXPERTS), jnp.uint32) >> 10) * slow
    expert = jnp.argsort(wait, axis=-1)[..., :TOP].astype(jnp.int32)
    chosen = jax.nn.one_hot(expert, EXPERTS, dtype=jnp.int32)
    in_line = jnp.cumsum(chosen.reshape(*devices, TOKENS * TOP, EXPERTS), axis=2) - 1
    slot = jnp.sum(in_line.reshape(chosen.shape) * chosen, axis=-1)

    def one(key, rows, columns):
        return (jax.random.normal(key, (rows, columns), jnp.float32) * rows**-0.5).astype(jnp.bfloat16)

    def weights(key, rows, columns):
        return jax.lax.map(lambda k: one(k, rows, columns), jax.random.split(key, EXPERTS))

    return {
        "x": jax.random.normal(kx, (*devices, TOKENS, D), jnp.float32).astype(jnp.bfloat16),
        "expert": expert,
        "slot": slot,
        "gate": jax.nn.softmax(jax.random.normal(kg, expert.shape, jnp.float32)),
        "w_gate": weights(k1, D, FF),
        "w_up": weights(k2, D, FF),
        "w_down": weights(k3, FF, D),
    }


def einsum(form, a, b):
    return jnp.einsum(form, a.astype(jnp.float32), b.astype(jnp.float32))


def reference(x, expert, slot, gate, w_gate, w_up, w_down):
    to_expert = jax.nn.one_hot(expert, EXPERTS, dtype=jnp.bfloat16)
    to_slot = jax.nn.one_hot(slot, SLOTS, dtype=jnp.bfloat16)
    weighted = to_expert * gate[..., None].astype(jnp.bfloat16)
    dispatch = einsum("abtke,abtkc->abtec", to_expert, to_slot).astype(jnp.bfloat16)
    combine = einsum("abtke,abtkc->abtec", weighted, to_slot).astype(jnp.bfloat16)
    z = einsum("abtec,abtd->aebcd", dispatch, x).astype(jnp.bfloat16)
    h = jax.nn.silu(einsum("aebcd,edf->aebcf", z, w_gate))
    h = (h * einsum("aebcd,edf->aebcf", z, w_up)).astype(jnp.bfloat16)
    out = einsum("aebcf,efd->aebcd", h, w_down).astype(jnp.bfloat16)
    y = einsum("abtec,aebcd->abtd", combine, out)
    return y.astype(jnp.bfloat16)
```

```python
import functools

import jax
import jax.numpy as jnp
from jax import lax
from jax.experimental import pallas as pl
from jax.experimental.pallas import tpu as pltpu
from jax.sharding import PartitionSpec as P

MESH = pl.DeviceIdType.MESH
BF = jnp.bfloat16
F32 = jnp.float32


def peer(me, r):
    x, y, c = me // 4, (me // 2) % 2, me % 2
    return ((x + r // 4) % 2) * 4 + ((y + (r // 2) % 2) % 2) * 2 + (c + r % 2) % 2


def block_of(o, r):
    a, b = slice(32 * r, 32 * r + 32), slice(256 + 8 * r, 264 + 8 * r)
    return jnp.concatenate([o[a, :256], o[b, :256], o[b, 256:], o[a, 256:]], axis=0).astype(BF)


def kernel(dims, x_ref, ex_ref, sl_ref, gt_ref, wg_ref, wu_ref, wd_ref, y_ref,
           x_buf, to_slots, weigh, send, z_in, back, z, acc, h, w_in, w_out,
           x_sem, in_sem, out_sem, send_sem, z_sem, back_send_sem, back_sem, y_sem):
    d, ff, chunks, slots, depth_in, depth_out = dims
    tokens = 256
    me = lax.axis_index("ep")

    def w_in_copy(e, k, m, slot):
        src = (wg_ref, wu_ref)[m]
        return pltpu.make_async_copy(src.at[e, pl.ds(k * 512, 512), :], w_in.at[slot], in_sem.at[slot])

    def w_out_copy(e, c, slot):
        return pltpu.make_async_copy(wd_ref.at[e, :, pl.ds(pl.multiple_of(c * 512, 512), 512)], w_out.at[slot],
                                     out_sem.at[slot])

    def x_copy(k):
        return pltpu.make_async_copy(x_ref.at[:, pl.ds(pl.multiple_of(k * 512, 512), 512)], x_buf.at[k], x_sem.at[k])

    barrier = pltpu.get_barrier_semaphore()
    for r in range(1, 8):
        pl.semaphore_signal(barrier, inc=1, device_id={"ep": peer(me, r)}, device_id_type=MESH)

    for k in range(chunks):
        x_copy(k).start()
    for i in range(depth_in):
        w_in_copy(0, i // 2, i % 2, i).start()
    for i in range(depth_out):
        w_out_copy(0, i, i).start()

    ex, sl = ex_ref[...], sl_ref[...]
    keep = sl < slots
    rel = jnp.bitwise_xor(ex // 2, me)
    half = ex % 2
    place = half * 320 + jnp.where(sl < 32, rel * 32 + sl, 256 + rel * 8 + sl - 32)
    place = jnp.where(keep, place, -1)
    p0, p1 = place[0:1, :], place[1:2, :]
    for e in range(2):
        row = lax.broadcasted_iota(jnp.int32, (320, tokens), 0) + 320 * e
        hit = jnp.where(row == p0, 1.0, jnp.where(row == p1, 1.0, 0.0))
        to_slots[e] = hit.astype(BF)

    pl.semaphore_wait(barrier, 7)

    def dispatch(i, _):
        e, k = i // chunks, i % chunks

        @pl.when(e == 0)
        def _():
            x_copy(k).wait()

        o = jnp.dot(to_slots[e], x_buf[k], preferred_element_type=F32)
        z_in[e, k, 0] = block_of(o, 0)
        for r in range(1, 8):
            send[e, k, r] = block_of(o, r)
        for r in (6, 2, 7, 3, 4, 5, 1):
            pltpu.make_async_remote_copy(
                src_ref=send.at[e, k, r], dst_ref=z_in.at[e, k, r], send_sem=send_sem.at[e], recv_sem=z_sem.at[e, k],
                device_id={"ep": peer(me, r)}, device_id_type=MESH).start()
        return 0

    lax.fori_loop(0, 2 * chunks, dispatch, 0)

    base = (half * 8 + rel) * 80
    left = jnp.where(keep, base + sl, -1).astype(F32)
    right = jnp.where(keep, base + jnp.where(sl < 32, 48 + sl, 8 + sl), -1).astype(F32)
    gt = gt_ref[...]
    rows = jnp.zeros((128, tokens), F32)
    line = lax.broadcasted_iota(jnp.int32, (128, tokens), 0)
    for i, v in enumerate((left[0:1], left[1:2], right[0:1], right[1:2], gt[0:1], gt[1:2])):
        rows = jnp.where(line == i, v, rows)
    down = rows.T
    col = lax.broadcasted_iota(jnp.int32, (tokens, 16 * 80), 1)
    for s in range(2):
        a0, a1 = (down[:, 2 * s + j:2 * s + j + 1].astype(jnp.int32) for j in range(2))
        weight = jnp.where(col == a0, down[:, 4:5], jnp.where(col == a1, down[:, 5:6], 0.0))
        weigh[s * tokens:(s + 1) * tokens, :] = weight.astype(BF)

    tiles = [(n, min(512, ff - n)) for n in range(0, ff, 512)]

    def clear(n, _):
        at = pl.ds(pl.multiple_of(n * 256, 256), 256)
        for m in range(2):
            acc[m, :, at] = jnp.zeros((320, 256), F32)
        return 0

    lax.fori_loop(0, ff // 256, clear, 0)

    def expert(e, _):
        def project(k, _):
            pltpu.make_async_copy(z_in.at[e, k, pl.ds(1, 7)], z_in.at[e, k, pl.ds(1, 7)], z_sem.at[e, k]).wait()
            for r in range(8):
                z[32 * r:32 * r + 32, 0:256] = z_in[e, k, r, 0:32, :]
                z[32 * r:32 * r + 32, 256:512] = z_in[e, k, r, 48:80, :]
            for r in range(0, 8, 2):
                a, b = z_in[e, k, r, 32:48, :].astype(F32), z_in[e, k, r + 1, 32:48, :].astype(F32)
                z[256 + 8 * r:272 + 8 * r, 0:256] = jnp.concatenate([a[:8], b[:8]], axis=0).astype(BF)
                z[256 + 8 * r:272 + 8 * r, 256:512] = jnp.concatenate([a[8:], b[8:]], axis=0).astype(BF)
            for m in range(2):
                i = (e * chunks + k) * 2 + m
                slot = i % depth_in
                w_in_copy(e, k, m, slot).wait()
                for n, w in tiles:
                    acc[m, :, n:n + w] += jnp.dot(z[...], w_in[slot, :, n:n + w], preferred_element_type=F32)
                later = i + depth_in
                for mm in range(2):
                    @pl.when(jnp.logical_and(later < 4 * chunks, later % 2 == mm))
                    def _():
                        w_in_copy(later // (2 * chunks), (later // 2) % chunks, mm, slot).start()
            return 0

        lax.fori_loop(0, chunks, project, 0)

        def activate(n, _):
            at = pl.ds(pl.multiple_of(n * 256, 256), 256)
            g, u = acc[0, :, at], acc[1, :, at]
            h[:, at] = (jax.nn.silu(g) * u).astype(BF)
            for m in range(2):
                acc[m, :, at] = jnp.zeros((320, 256), F32)
            return 0

        lax.fori_loop(0, ff // 256, activate, 0)

        pltpu.make_async_copy(send.at[e, :, pl.ds(1, 7)], send.at[e, :, pl.ds(1, 7)], send_sem.at[e]).wait()

        def finish(c, _):
            j = e * chunks + c
            slot = j % depth_out
            w_out_copy(e, c, slot).wait()
            o = jnp.dot(h[...], w_out[slot], preferred_element_type=F32)
            back[c, e, 0] = block_of(o, 0)
            for r in range(1, 8):
                send[e, c, r] = block_of(o, r)
            later = j + depth_out

            @pl.when(later < 2 * chunks)
            def _():
                w_out_copy(later // chunks, later % chunks, slot).start()

            for r in (6, 2, 7, 3, 4, 5, 1):
                pltpu.make_async_remote_copy(
                    src_ref=send.at[e, c, r], dst_ref=back.at[c, e, r], send_sem=back_send_sem.at[e],
                    recv_sem=back_sem.at[e, c], device_id={"ep": peer(me, r)}, device_id_type=MESH).start()
            return 0

        lax.fori_loop(0, chunks, finish, 0)
        return 0

    lax.fori_loop(0, 2, expert, 0)

    def y_copy(c, at):
        return pltpu.make_async_copy(x_buf.at[c], y_ref.at[:, pl.ds(pl.multiple_of(c * 512, 512), 512)], y_sem.at[at])

    def gather(c, _):
        for e in range(2):
            pltpu.make_async_copy(back.at[c, e, pl.ds(1, 7)], back.at[c, e, pl.ds(1, 7)], back_sem.at[e, c]).wait()
        o = jnp.dot(weigh[...], back[c].reshape(16 * 80, 256), preferred_element_type=F32)
        x_buf[c, :, 0:256] = o[:tokens].astype(BF)
        x_buf[c, :, 256:512] = o[tokens:].astype(BF)
        y_copy(c, c).start()
        return 0

    lax.fori_loop(0, chunks, gather, 0)
    for c in range(chunks):
        y_copy(c, c).wait()
    for e in range(2):
        pltpu.make_async_copy(send.at[e, :, pl.ds(1, 7)], send.at[e, :, pl.ds(1, 7)], back_send_sem.at[e]).wait()


def solution(mesh):
    def local(x, expert, slot, gate, w_gate, w_up, w_down):
        tokens, d = x.shape[2:]
        ff = w_gate.shape[2]
        top = expert.shape[3]
        chunks = d // 512
        slots = 5 * tokens * top // (4 * 8 * w_gate.shape[0])
        depth_in, depth_out = 3, 3
        anywhere = pl.BlockSpec(memory_space=pl.ANY)
        vmem = pl.BlockSpec(memory_space=pltpu.VMEM)
        y = pl.pallas_call(
            functools.partial(kernel, (d, ff, chunks, slots, depth_in, depth_out)),
            out_shape=jax.ShapeDtypeStruct((tokens, d), BF),
            in_specs=[anywhere, vmem, vmem, vmem, anywhere, anywhere, anywhere],
            out_specs=anywhere,
            scratch_shapes=[
                pltpu.VMEM((chunks, tokens, 512), BF),
                pltpu.VMEM((2, 320, tokens), BF),
                pltpu.VMEM((2 * tokens, 16 * 80), BF),
                pltpu.VMEM((2, chunks, 8, 80, 256), BF),
                pltpu.VMEM((2, chunks, 8, 80, 256), BF),
                pltpu.VMEM((chunks, 2, 8, 80, 256), BF),
                pltpu.VMEM((320, 512), BF),
                pltpu.VMEM((2, 320, ff), F32),
                pltpu.VMEM((320, ff), BF),
                pltpu.VMEM((depth_in, 512, ff), BF),
                pltpu.VMEM((depth_out, ff, 512), BF),
                pltpu.SemaphoreType.DMA((chunks,)),
                pltpu.SemaphoreType.DMA((depth_in,)),
                pltpu.SemaphoreType.DMA((depth_out,)),
                pltpu.SemaphoreType.DMA((2,)),
                pltpu.SemaphoreType.DMA((2, chunks)),
                pltpu.SemaphoreType.DMA((2,)),
                pltpu.SemaphoreType.DMA((2, chunks)),
                pltpu.SemaphoreType.DMA((chunks,)),
            ],
            compiler_params=pltpu.CompilerParams(collective_id=0, has_side_effects=True,
                                                 vmem_limit_bytes=67043328),
        )(x.reshape(tokens, d), expert.reshape(tokens, top).T, slot.reshape(tokens, top).T,
          gate.reshape(tokens, top).T,
          w_gate, w_up, w_down)
        return y.reshape(x.shape)

    tok = P("dp", "ep", None, None)
    wts = P("ep", None, None)
    return jax.shard_map(local, mesh=mesh, in_specs=(tok, tok, tok, tok, wts, wts, wts), out_specs=tok,
                         check_vma=False)
```

```python
import functools

import jax
import jax.numpy as jnp
from jax import lax
from jax.experimental import pallas as pl
from jax.experimental.pallas import tpu as pltpu
from jax.sharding import PartitionSpec as P

MESH = pl.DeviceIdType.MESH
BF = jnp.bfloat16
F32 = jnp.float32


def peer(me, r):
    x, y, c = me // 4, (me // 2) % 2, me % 2
    return ((x + r // 4) % 2) * 4 + ((y + (r // 2) % 2) % 2) * 2 + (c + r % 2) % 2


def block_of(o, r):
    a, b = slice(32 * r, 32 * r + 32), slice(256 + 8 * r, 264 + 8 * r)
    return jnp.concatenate([o[a, :256], o[b, :256], o[b, 256:], o[a, 256:]], axis=0).astype(BF)


def kernel(dims, x_ref, ex_ref, sl_ref, gt_ref, wg_ref, wu_ref, wd_ref, y_ref,
           x_buf, to_slots, weigh, send, z_in, back, z, acc, h, w_in, w_out,
           x_sem, in_sem, out_sem, send_sem, z_sem, back_send_sem, back_sem, y_sem):
    d, ff, chunks, slots, depth_in, depth_out = dims
    tokens = 256
    me = lax.axis_index("ep")

    def w_in_copy(e, k, m, slot):
        src = (wg_ref, wu_ref)[m]
        return pltpu.make_async_copy(src.at[e, pl.ds(k * 512, 512), :], w_in.at[slot], in_sem.at[slot])

    def w_out_copy(e, c, slot):
        return pltpu.make_async_copy(wd_ref.at[e, :, pl.ds(pl.multiple_of(c * 512, 512), 512)], w_out.at[slot],
                                     out_sem.at[slot])

    def x_copy(k):
        return pltpu.make_async_copy(x_ref.at[:, pl.ds(pl.multiple_of(k * 512, 512), 512)], x_buf.at[k], x_sem.at[k])

    barrier = pltpu.get_barrier_semaphore()
    for r in range(1, 8):
        pl.semaphore_signal(barrier, inc=1, device_id={"ep": peer(me, r)}, device_id_type=MESH)

    for k in range(chunks):
        x_copy(k).start()

    ex, sl = ex_ref[...], sl_ref[...]
    keep = sl < slots
    rel = jnp.bitwise_xor(ex // 2, me)
    half = ex % 2
    place = half * 320 + jnp.where(sl < 32, rel * 32 + sl, 256 + rel * 8 + sl - 32)
    place = jnp.where(keep, place, -1)
    p0, p1 = place[0:1, :], place[1:2, :]
    for e in range(2):
        row = lax.broadcasted_iota(jnp.int32, (320, tokens), 0) + 320 * e
        hit = jnp.where(row == p0, 1.0, jnp.where(row == p1, 1.0, 0.0))
        to_slots[e] = hit.astype(BF)

    for k in range(chunks):
        x_copy(k).wait()
    for i in range(depth_in):
        w_in_copy(0, i // 2, i % 2, i).start()
    pl.semaphore_wait(barrier, 7)

    def dispatch(i, _):
        e, k = i // chunks, i % chunks
        o = jnp.dot(to_slots[e], x_buf[k], preferred_element_type=F32)
        z_in[e, k, 0] = block_of(o, 0)
        for r in range(1, 8):
            send[e, k, r] = block_of(o, r)
        for r in (6, 2, 7, 3, 4, 5, 1):
            pltpu.make_async_remote_copy(
                src_ref=send.at[e, k, r], dst_ref=z_in.at[e, k, r], send_sem=send_sem.at[e], recv_sem=z_sem.at[e, k],
                device_id={"ep": peer(me, r)}, device_id_type=MESH).start()
        return 0

    lax.fori_loop(0, 2 * chunks, dispatch, 0)

    for i in range(depth_out):
        w_out_copy(0, i, i).start()

    tiles = [(n, min(512, ff - n)) for n in range(0, ff, 512)]

    def expert(e, _):
        def project(k, _):
            pltpu.make_async_copy(z_in.at[e, k, pl.ds(1, 7)], z_in.at[e, k, pl.ds(1, 7)], z_sem.at[e, k]).wait()
            for r in range(8):
                z[32 * r:32 * r + 32, 0:256] = z_in[e, k, r, 0:32, :]
                z[32 * r:32 * r + 32, 256:512] = z_in[e, k, r, 48:80, :]
            for r in range(0, 8, 2):
                a, b = z_in[e, k, r, 32:48, :].astype(F32), z_in[e, k, r + 1, 32:48, :].astype(F32)
                z[256 + 8 * r:272 + 8 * r, 0:256] = jnp.concatenate([a[:8], b[:8]], axis=0).astype(BF)
                z[256 + 8 * r:272 + 8 * r, 256:512] = jnp.concatenate([a[8:], b[8:]], axis=0).astype(BF)
            for m in range(2):
                i = (e * chunks + k) * 2 + m
                slot = i % depth_in
                w_in_copy(e, k, m, slot).wait()
                for n, w in tiles:
                    part = jnp.dot(z[...], w_in[slot, :, n:n + w], preferred_element_type=F32)
                    acc[m, :, n:n + w] = jnp.where(k == 0, 0.0, acc[m, :, n:n + w]) + part
                later = i + depth_in
                for mm in range(2):
                    @pl.when(jnp.logical_and(later < 4 * chunks, later % 2 == mm))
                    def _():
                        w_in_copy(later // (2 * chunks), (later // 2) % chunks, mm, slot).start()
            return 0

        lax.fori_loop(0, chunks, project, 0)

        def activate(n, _):
            at = pl.ds(pl.multiple_of(n * 256, 256), 256)
            g, u = acc[0, :, at], acc[1, :, at]
            h[:, at] = (jax.nn.silu(g) * u).astype(BF)
            return 0

        lax.fori_loop(0, ff // 256, activate, 0)

        pltpu.make_async_copy(send.at[e, :, pl.ds(1, 7)], send.at[e, :, pl.ds(1, 7)], send_sem.at[e]).wait()

        def finish(c, _):
            j = e * chunks + c
            slot = j % depth_out
            w_out_copy(e, c, slot).wait()
            o = jnp.dot(h[...], w_out[slot], preferred_element_type=F32)
            back[c, e, 0] = block_of(o, 0)
            for r in range(1, 8):
                send[e, c, r] = block_of(o, r)
            later = j + depth_out

            @pl.when(later < 2 * chunks)
            def _():
                w_out_copy(later // chunks, later % chunks, slot).start()

            for r in (6, 2, 7, 3, 4, 5, 1):
                pltpu.make_async_remote_copy(
                    src_ref=send.at[e, c, r], dst_ref=back.at[c, e, r], send_sem=back_send_sem.at[e],
                    recv_sem=back_sem.at[e, c], device_id={"ep": peer(me, r)}, device_id_type=MESH).start()
            return 0

        lax.fori_loop(0, chunks, finish, 0)
        return 0

    lax.fori_loop(0, 2, expert, 0)

    base = (half * 8 + rel) * 80
    left = jnp.where(keep, base + sl, -1).astype(F32)
    right = jnp.where(keep, base + jnp.where(sl < 32, 48 + sl, 8 + sl), -1).astype(F32)
    gt = gt_ref[...]
    rows = jnp.zeros((128, tokens), F32)
    line = lax.broadcasted_iota(jnp.int32, (128, tokens), 0)
    for i, v in enumerate((left[0:1], left[1:2], right[0:1], right[1:2], gt[0:1], gt[1:2])):
        rows = jnp.where(line == i, v, rows)
    down = rows.T
    col = lax.broadcasted_iota(jnp.int32, (tokens, 16 * 80), 1)
    for s in range(2):
        a0, a1 = (down[:, 2 * s + j:2 * s + j + 1].astype(jnp.int32) for j in range(2))
        weight = jnp.where(col == a0, down[:, 4:5], jnp.where(col == a1, down[:, 5:6], 0.0))
        weigh[s * tokens:(s + 1) * tokens, :] = weight.astype(BF)

    def y_copy(c, at):
        return pltpu.make_async_copy(x_buf.at[c], y_ref.at[:, pl.ds(pl.multiple_of(c * 512, 512), 512)], y_sem.at[at])

    def gather(c, _):
        for e in range(2):
            pltpu.make_async_copy(back.at[c, e, pl.ds(1, 7)], back.at[c, e, pl.ds(1, 7)], back_sem.at[e, c]).wait()
        o = jnp.dot(weigh[...], back[c].reshape(16 * 80, 256), preferred_element_type=F32)
        x_buf[c, :, 0:256] = o[:tokens].astype(BF)
        x_buf[c, :, 256:512] = o[tokens:].astype(BF)
        y_copy(c, c).start()
        return 0

    lax.fori_loop(0, chunks, gather, 0)
    for c in range(chunks):
        y_copy(c, c).wait()
    for e in range(2):
        pltpu.make_async_copy(send.at[e, :, pl.ds(1, 7)], send.at[e, :, pl.ds(1, 7)], back_send_sem.at[e]).wait()


def solution(mesh):
    def local(x, expert, slot, gate, w_gate, w_up, w_down):
        tokens, d = x.shape[2:]
        ff = w_gate.shape[2]
        top = expert.shape[3]
        chunks = d // 512
        slots = 5 * tokens * top // (4 * 8 * w_gate.shape[0])
        depth_in, depth_out = 3, 3
        anywhere = pl.BlockSpec(memory_space=pl.ANY)
        vmem = pl.BlockSpec(memory_space=pltpu.VMEM)
        y = pl.pallas_call(
            functools.partial(kernel, (d, ff, chunks, slots, depth_in, depth_out)),
            out_shape=jax.ShapeDtypeStruct((tokens, d), BF),
            in_specs=[anywhere, vmem, vmem, vmem, anywhere, anywhere, anywhere],
            out_specs=anywhere,
            scratch_shapes=[
                pltpu.VMEM((chunks, tokens, 512), BF),
                pltpu.VMEM((2, 320, tokens), BF),
                pltpu.VMEM((2 * tokens, 16 * 80), BF),
                pltpu.VMEM((2, chunks, 8, 80, 256), BF),
                pltpu.VMEM((2, chunks, 8, 80, 256), BF),
                pltpu.VMEM((chunks, 2, 8, 80, 256), BF),
                pltpu.VMEM((320, 512), BF),
                pltpu.VMEM((2, 320, ff), F32),
                pltpu.VMEM((320, ff), BF),
                pltpu.VMEM((depth_in, 512, ff), BF),
                pltpu.VMEM((depth_out, ff, 512), BF),
                pltpu.SemaphoreType.DMA((chunks,)),
                pltpu.SemaphoreType.DMA((depth_in,)),
                pltpu.SemaphoreType.DMA((depth_out,)),
                pltpu.SemaphoreType.DMA((2,)),
                pltpu.SemaphoreType.DMA((2, chunks)),
                pltpu.SemaphoreType.DMA((2,)),
                pltpu.SemaphoreType.DMA((2, chunks)),
                pltpu.SemaphoreType.DMA((chunks,)),
            ],
            compiler_params=pltpu.CompilerParams(collective_id=0, has_side_effects=True,
                                                 vmem_limit_bytes=67043328),
        )(x.reshape(tokens, d), expert.reshape(tokens, top).T, slot.reshape(tokens, top).T,
          gate.reshape(tokens, top).T,
          w_gate, w_up, w_down)
        return y.reshape(x.shape)

    tok = P("dp", "ep", None, None)
    wts = P("ep", None, None)
    return jax.shard_map(local, mesh=mesh, in_specs=(tok, tok, tok, tok, wts, wts, wts), out_specs=tok,
                         check_vma=False)
```

```python
import functools

import jax
import jax.numpy as jnp
from jax import lax
from jax.experimental import pallas as pl
from jax.experimental.pallas import tpu as pltpu
from jax.sharding import PartitionSpec as P

MESH = pl.DeviceIdType.MESH
BF = jnp.bfloat16
F32 = jnp.float32


def peer(me, r):
    x, y, c = me // 4, (me // 2) % 2, me % 2
    return ((x + r // 4) % 2) * 4 + ((y + (r // 2) % 2) % 2) * 2 + (c + r % 2) % 2


def block_of(o, r):
    a, b = slice(32 * r, 32 * r + 32), slice(256 + 8 * r, 264 + 8 * r)
    return jnp.concatenate([o[a, :256], o[b, :256], o[b, 256:], o[a, 256:]], axis=0).astype(BF)


def kernel(dims, x_ref, ex_ref, sl_ref, gt_ref, wg_ref, wu_ref, wd_ref, y_ref,
           x_buf, to_slots, weigh, send, z_in, back, z, acc, h, w_in, w_out,
           x_sem, in_sem, out_sem, send_sem, z_sem, back_send_sem, back_sem, y_sem):
    d, ff, chunks, slots, depth_in, depth_out = dims
    tokens = 256
    me = lax.axis_index("ep")

    def w_in_copy(e, k, m, slot):
        src = (wg_ref, wu_ref)[m]
        return pltpu.make_async_copy(src.at[e, pl.ds(k * 512, 512), :], w_in.at[slot], in_sem.at[slot])

    def w_out_copy(e, c, slot):
        return pltpu.make_async_copy(wd_ref.at[e, :, pl.ds(pl.multiple_of(c * 512, 512), 512)], w_out.at[slot],
                                     out_sem.at[slot])

    def x_copy(k):
        return pltpu.make_async_copy(x_ref.at[:, pl.ds(pl.multiple_of(k * 512, 512), 512)], x_buf.at[k], x_sem.at[k])

    barrier = pltpu.get_barrier_semaphore()
    for r in range(1, 8):
        pl.semaphore_signal(barrier, inc=1, device_id={"ep": peer(me, r)}, device_id_type=MESH)

    for k in range(chunks):
        x_copy(k).start()

    ex, sl = ex_ref[...], sl_ref[...]
    keep = sl < slots
    rel = jnp.bitwise_xor(ex // 2, me)
    half = ex % 2
    place = half * 320 + jnp.where(sl < 32, rel * 32 + sl, 256 + rel * 8 + sl - 32)
    place = jnp.where(keep, place, -1)
    p0, p1 = place[0:1, :], place[1:2, :]
    for e in range(2):
        row = lax.broadcasted_iota(jnp.int32, (320, tokens), 0) + 320 * e
        hit = jnp.where(row == p0, 1.0, jnp.where(row == p1, 1.0, 0.0))
        to_slots[e] = hit.astype(BF)

    for k in range(chunks):
        x_copy(k).wait()
    for i in range(depth_in):
        w_in_copy(0, i // 2, i % 2, i).start()
    pl.semaphore_wait(barrier, 7)

    def dispatch(i, _):
        e, k = i // chunks, i % chunks
        o = jnp.dot(to_slots[e], x_buf[k], preferred_element_type=F32)
        z_in[e, k, 0] = block_of(o, 0)
        for r in range(1, 8):
            send[e, k, r] = block_of(o, r)
        for r in (6, 2, 7, 3, 4, 5, 1):
            pltpu.make_async_remote_copy(
                src_ref=send.at[e, k, r], dst_ref=z_in.at[e, k, r], send_sem=send_sem.at[e], recv_sem=z_sem.at[e, k],
                device_id={"ep": peer(me, r)}, device_id_type=MESH).start()
        return 0

    lax.fori_loop(0, 2 * chunks, dispatch, 0)

    for i in range(depth_out):
        w_out_copy(0, i, i).start()

    tiles = [(slice(0, 320), n, 512) for n in range(0, ff - 511, 512)]
    tiles += [(slice(m, m + 160), ff - 256, 256) for m in (0, 160)]

    def expert(e, _):
        def project(k, last):
            pltpu.make_async_copy(z_in.at[e, k, pl.ds(1, 7)], z_in.at[e, k, pl.ds(1, 7)], z_sem.at[e, k]).wait()
            for r in range(8):
                z[32 * r:32 * r + 32, 0:256] = z_in[e, k, r, 0:32, :]
                z[32 * r:32 * r + 32, 256:512] = z_in[e, k, r, 48:80, :]
            for r in range(0, 8, 2):
                a, b = z_in[e, k, r, 32:48, :].astype(F32), z_in[e, k, r + 1, 32:48, :].astype(F32)
                z[256 + 8 * r:272 + 8 * r, 0:256] = jnp.concatenate([a[:8], b[:8]], axis=0).astype(BF)
                z[256 + 8 * r:272 + 8 * r, 256:512] = jnp.concatenate([a[8:], b[8:]], axis=0).astype(BF)
            for m in range(2):
                i = (e * chunks + k) * 2 + m
                slot = i % depth_in
                w_in_copy(e, k, m, slot).wait()
                for rows, n, w in tiles:
                    at = slice(n, n + w)
                    part = jnp.dot(z[rows, :], w_in[slot, :, at], preferred_element_type=F32)
                    if not last:
                        acc[m, rows, at] = jnp.where(k == 0, 0.0, acc[m, rows, at]) + part
                    elif m == 0:
                        acc[0, rows, at] += part
                    else:
                        g, u = acc[0, rows, at], acc[1, rows, at] + part
                        h[rows, at] = (jax.nn.silu(g) * u).astype(BF)
                later = i + depth_in
                for mm in range(2):
                    @pl.when(jnp.logical_and(later < 4 * chunks, later % 2 == mm))
                    def _():
                        w_in_copy(later // (2 * chunks), (later // 2) % chunks, mm, slot).start()
            return 0

        lax.fori_loop(0, chunks - 1, lambda k, _: project(k, False), 0)
        project(chunks - 1, True)

        pltpu.make_async_copy(send.at[e, :, pl.ds(1, 7)], send.at[e, :, pl.ds(1, 7)], send_sem.at[e]).wait()

        def finish(c, _):
            j = e * chunks + c
            slot = j % depth_out
            w_out_copy(e, c, slot).wait()
            o = jnp.dot(h[...], w_out[slot], preferred_element_type=F32)
            back[c, e, 0] = block_of(o, 0)
            for r in range(1, 8):
                send[e, c, r] = block_of(o, r)
            later = j + depth_out

            @pl.when(later < 2 * chunks)
            def _():
                w_out_copy(later // chunks, later % chunks, slot).start()

            for r in (6, 2, 7, 3, 4, 5, 1):
                pltpu.make_async_remote_copy(
                    src_ref=send.at[e, c, r], dst_ref=back.at[c, e, r], send_sem=back_send_sem.at[e],
                    recv_sem=back_sem.at[e, c], device_id={"ep": peer(me, r)}, device_id_type=MESH).start()
            return 0

        lax.fori_loop(0, chunks, finish, 0)
        return 0

    lax.fori_loop(0, 2, expert, 0)

    base = (half * 8 + rel) * 80
    left = jnp.where(keep, base + sl, -1).astype(F32)
    right = jnp.where(keep, base + jnp.where(sl < 32, 48 + sl, 8 + sl), -1).astype(F32)
    gt = gt_ref[...]
    rows = jnp.zeros((128, tokens), F32)
    line = lax.broadcasted_iota(jnp.int32, (128, tokens), 0)
    for i, v in enumerate((left[0:1], left[1:2], right[0:1], right[1:2], gt[0:1], gt[1:2])):
        rows = jnp.where(line == i, v, rows)
    down = rows.T
    col = lax.broadcasted_iota(jnp.int32, (tokens, 16 * 80), 1)
    for s in range(2):
        a0, a1 = (down[:, 2 * s + j:2 * s + j + 1].astype(jnp.int32) for j in range(2))
        weight = jnp.where(col == a0, down[:, 4:5], jnp.where(col == a1, down[:, 5:6], 0.0))
        weigh[s * tokens:(s + 1) * tokens, :] = weight.astype(BF)

    def y_copy(c, at):
        return pltpu.make_async_copy(x_buf.at[c], y_ref.at[:, pl.ds(pl.multiple_of(c * 512, 512), 512)], y_sem.at[at])

    def gather(c, _):
        for e in range(2):
            pltpu.make_async_copy(back.at[c, e, pl.ds(1, 7)], back.at[c, e, pl.ds(1, 7)], back_sem.at[e, c]).wait()
        o = jnp.dot(weigh[...], back[c].reshape(16 * 80, 256), preferred_element_type=F32)
        x_buf[c, :, 0:256] = o[:tokens].astype(BF)
        x_buf[c, :, 256:512] = o[tokens:].astype(BF)
        y_copy(c, c).start()
        return 0

    lax.fori_loop(0, chunks, gather, 0)
    for c in range(chunks):
        y_copy(c, c).wait()
    for e in range(2):
        pltpu.make_async_copy(send.at[e, :, pl.ds(1, 7)], send.at[e, :, pl.ds(1, 7)], back_send_sem.at[e]).wait()


def solution(mesh):
    def local(x, expert, slot, gate, w_gate, w_up, w_down):
        tokens, d = x.shape[2:]
        ff = w_gate.shape[2]
        top = expert.shape[3]
        chunks = d // 512
        slots = 5 * tokens * top // (4 * 8 * w_gate.shape[0])
        depth_in, depth_out = 3, 3
        anywhere = pl.BlockSpec(memory_space=pl.ANY)
        vmem = pl.BlockSpec(memory_space=pltpu.VMEM)
        y = pl.pallas_call(
            functools.partial(kernel, (d, ff, chunks, slots, depth_in, depth_out)),
            out_shape=jax.ShapeDtypeStruct((tokens, d), BF),
            in_specs=[anywhere, vmem, vmem, vmem, anywhere, anywhere, anywhere],
            out_specs=anywhere,
            scratch_shapes=[
                pltpu.VMEM((chunks, tokens, 512), BF),
                pltpu.VMEM((2, 320, tokens), BF),
                pltpu.VMEM((2 * tokens, 16 * 80), BF),
                pltpu.VMEM((2, chunks, 8, 80, 256), BF),
                pltpu.VMEM((2, chunks, 8, 80, 256), BF),
                pltpu.VMEM((chunks, 2, 8, 80, 256), BF),
                pltpu.VMEM((320, 512), BF),
                pltpu.VMEM((2, 320, ff), F32),
                pltpu.VMEM((320, ff), BF),
                pltpu.VMEM((depth_in, 512, ff), BF),
                pltpu.VMEM((depth_out, ff, 512), BF),
                pltpu.SemaphoreType.DMA((chunks,)),
                pltpu.SemaphoreType.DMA((depth_in,)),
                pltpu.SemaphoreType.DMA((depth_out,)),
                pltpu.SemaphoreType.DMA((2,)),
                pltpu.SemaphoreType.DMA((2, chunks)),
                pltpu.SemaphoreType.DMA((2,)),
                pltpu.SemaphoreType.DMA((2, chunks)),
                pltpu.SemaphoreType.DMA((chunks,)),
            ],
            compiler_params=pltpu.CompilerParams(collective_id=0, has_side_effects=True,
                                                 vmem_limit_bytes=67043328),
        )(x.reshape(tokens, d), expert.reshape(tokens, top).T, slot.reshape(tokens, top).T,
          gate.reshape(tokens, top).T,
          w_gate, w_up, w_down)
        return y.reshape(x.shape)

    tok = P("dp", "ep", None, None)
    wts = P("ep", None, None)
    return jax.shard_map(local, mesh=mesh, in_specs=(tok, tok, tok, tok, wts, wts, wts), out_specs=tok,
                         check_vma=False)
```

```python
import functools

import jax
import jax.numpy as jnp
from jax import lax
from jax.experimental import pallas as pl
from jax.experimental.pallas import tpu as pltpu
from jax.sharding import PartitionSpec as P

MESH = pl.DeviceIdType.MESH
BF = jnp.bfloat16
F32 = jnp.float32


def peer(me, r):
    x, y, c = me // 4, (me // 2) % 2, me % 2
    return ((x + r // 4) % 2) * 4 + ((y + (r // 2) % 2) % 2) * 2 + (c + r % 2) % 2


def block_of(o, r):
    a, b = slice(32 * r, 32 * r + 32), slice(256 + 8 * r, 264 + 8 * r)
    return jnp.concatenate([o[a, :256], o[b, :256], o[b, 256:], o[a, 256:]], axis=0).astype(BF)


def kernel(dims, x_ref, ex_ref, sl_ref, gt_ref, wg_ref, wu_ref, wd_ref, y_ref,
           x_buf, to_slots, weigh, send, z_in, back, z, acc, h, w_in, w_out,
           x_sem, in_sem, out_sem, send_sem, z_sem, back_send_sem, back_sem, y_sem):
    d, ff, chunks, slots, depth_in, depth_out = dims
    tokens = 256
    me = lax.axis_index("ep")

    def w_in_copy(e, k, m, slot):
        src = (wg_ref, wu_ref)[m]
        return pltpu.make_async_copy(src.at[e, pl.ds(k * 512, 512), :], w_in.at[slot], in_sem.at[slot])

    def w_out_copy(e, c, slot):
        return pltpu.make_async_copy(wd_ref.at[e, :, pl.ds(pl.multiple_of(c * 512, 512), 512)], w_out.at[slot],
                                     out_sem.at[slot])

    def x_copy(k):
        return pltpu.make_async_copy(x_ref.at[:, pl.ds(pl.multiple_of(k * 512, 512), 512)], x_buf.at[k], x_sem.at[k])

    barrier = pltpu.get_barrier_semaphore()
    for r in range(1, 8):
        pl.semaphore_signal(barrier, inc=1, device_id={"ep": peer(me, r)}, device_id_type=MESH)

    for k in range(chunks):
        x_copy(k).start()

    ex, sl = ex_ref[...], sl_ref[...]
    keep = sl < slots
    rel = jnp.bitwise_xor(ex // 2, me)
    half = ex % 2
    place = half * 320 + jnp.where(sl < 32, rel * 32 + sl, 256 + rel * 8 + sl - 32)
    place = jnp.where(keep, place, -1)
    p0, p1 = place[0:1, :], place[1:2, :]
    for e in range(2):
        row = lax.broadcasted_iota(jnp.int32, (320, tokens), 0) + 320 * e
        hit = jnp.where(row == p0, 1.0, jnp.where(row == p1, 1.0, 0.0))
        to_slots[e] = hit.astype(BF)

    pl.semaphore_wait(barrier, 7)

    def dispatch(i, _):
        e, k = i // chunks, i % chunks

        @pl.when(e == 0)
        def _():
            x_copy(k).wait()

        o = jnp.dot(to_slots[e], x_buf[k], preferred_element_type=F32)
        z_in[e, k, 0] = block_of(o, 0)
        for r in range(1, 8):
            send[e, k, r] = block_of(o, r)
        for r in (6, 2, 7, 3, 4, 5, 1):
            pltpu.make_async_remote_copy(
                src_ref=send.at[e, k, r], dst_ref=z_in.at[e, k, r], send_sem=send_sem.at[e], recv_sem=z_sem.at[e, k],
                device_id={"ep": peer(me, r)}, device_id_type=MESH).start()

        @pl.when(i == 2)
        def _():
            for j in range(depth_in):
                w_in_copy(0, j // 2, j % 2, j).start()

        return 0

    lax.fori_loop(0, 2 * chunks, dispatch, 0)

    for i in range(depth_out):
        w_out_copy(0, i, i).start()

    tiles = [(slice(0, 320), n, 512) for n in range(0, ff - 511, 512)]
    tiles += [(slice(m, m + 160), ff - 256, 256) for m in (0, 160)]

    def expert(e, _):
        def project(k, last):
            pltpu.make_async_copy(z_in.at[e, k, pl.ds(1, 7)], z_in.at[e, k, pl.ds(1, 7)], z_sem.at[e, k]).wait()
            for r in range(8):
                z[32 * r:32 * r + 32, 0:256] = z_in[e, k, r, 0:32, :]
                z[32 * r:32 * r + 32, 256:512] = z_in[e, k, r, 48:80, :]
            for r in range(0, 8, 2):
                a, b = z_in[e, k, r, 32:48, :].astype(F32), z_in[e, k, r + 1, 32:48, :].astype(F32)
                z[256 + 8 * r:272 + 8 * r, 0:256] = jnp.concatenate([a[:8], b[:8]], axis=0).astype(BF)
                z[256 + 8 * r:272 + 8 * r, 256:512] = jnp.concatenate([a[8:], b[8:]], axis=0).astype(BF)
            for m in range(2):
                i = (e * chunks + k) * 2 + m
                slot = i % depth_in
                w_in_copy(e, k, m, slot).wait()
                for rows, n, w in tiles:
                    at = slice(n, n + w)
                    part = jnp.dot(z[rows, :], w_in[slot, :, at], preferred_element_type=F32)
                    if not last:
                        acc[m, rows, at] = jnp.where(k == 0, 0.0, acc[m, rows, at]) + part
                    elif m == 0:
                        acc[0, rows, at] += part
                    else:
                        g, u = acc[0, rows, at], acc[1, rows, at] + part
                        h[rows, at] = (jax.nn.silu(g) * u).astype(BF)
                later = i + depth_in
                for mm in range(2):
                    @pl.when(jnp.logical_and(later < 4 * chunks, later % 2 == mm))
                    def _():
                        w_in_copy(later // (2 * chunks), (later // 2) % chunks, mm, slot).start()
            return 0

        lax.fori_loop(0, chunks - 1, lambda k, _: project(k, False), 0)
        project(chunks - 1, True)

        pltpu.make_async_copy(send.at[e, :, pl.ds(1, 7)], send.at[e, :, pl.ds(1, 7)], send_sem.at[e]).wait()

        def finish(c, _):
            j = e * chunks + c
            slot = j % depth_out
            w_out_copy(e, c, slot).wait()
            o = jnp.dot(h[...], w_out[slot], preferred_element_type=F32)
            back[c, e, 0] = block_of(o, 0)
            for r in range(1, 8):
                send[e, c, r] = block_of(o, r)
            later = j + depth_out

            @pl.when(later < 2 * chunks)
            def _():
                w_out_copy(later // chunks, later % chunks, slot).start()

            for r in (6, 2, 7, 3, 4, 5, 1):
                pltpu.make_async_remote_copy(
                    src_ref=send.at[e, c, r], dst_ref=back.at[c, e, r], send_sem=back_send_sem.at[e],
                    recv_sem=back_sem.at[e, c], device_id={"ep": peer(me, r)}, device_id_type=MESH).start()
            return 0

        lax.fori_loop(0, chunks, finish, 0)
        return 0

    lax.fori_loop(0, 2, expert, 0)

    base = (half * 8 + rel) * 80
    left = jnp.where(keep, base + sl, -1).astype(F32)
    right = jnp.where(keep, base + jnp.where(sl < 32, 48 + sl, 8 + sl), -1).astype(F32)
    gt = gt_ref[...]
    rows = jnp.zeros((128, tokens), F32)
    line = lax.broadcasted_iota(jnp.int32, (128, tokens), 0)
    for i, v in enumerate((left[0:1], left[1:2], right[0:1], right[1:2], gt[0:1], gt[1:2])):
        rows = jnp.where(line == i, v, rows)
    down = rows.T
    col = lax.broadcasted_iota(jnp.int32, (tokens, 16 * 80), 1)
    for s in range(2):
        a0, a1 = (down[:, 2 * s + j:2 * s + j + 1].astype(jnp.int32) for j in range(2))
        weight = jnp.where(col == a0, down[:, 4:5], jnp.where(col == a1, down[:, 5:6], 0.0))
        weigh[s * tokens:(s + 1) * tokens, :] = weight.astype(BF)

    def y_copy(c, at):
        return pltpu.make_async_copy(x_buf.at[c], y_ref.at[:, pl.ds(pl.multiple_of(c * 512, 512), 512)], y_sem.at[at])

    def gather(c, _):
        for e in range(2):
            pltpu.make_async_copy(back.at[c, e, pl.ds(1, 7)], back.at[c, e, pl.ds(1, 7)], back_sem.at[e, c]).wait()
        o = jnp.dot(weigh[...], back[c].reshape(16 * 80, 256), preferred_element_type=F32)
        x_buf[c, :, 0:256] = o[:tokens].astype(BF)
        x_buf[c, :, 256:512] = o[tokens:].astype(BF)
        y_copy(c, c).start()
        return 0

    lax.fori_loop(0, chunks, gather, 0)
    for c in range(chunks):
        y_copy(c, c).wait()
    for e in range(2):
        pltpu.make_async_copy(send.at[e, :, pl.ds(1, 7)], send.at[e, :, pl.ds(1, 7)], back_send_sem.at[e]).wait()


def settle(pieces, a_ref, o_ref, buf, in_sem, out_sem):
    width = a_ref.shape[1] // pieces
    at = [pl.ds(i * width, width) for i in range(pieces)]
    reads = [pltpu.make_async_copy(a_ref.at[:, s], buf.at[i], in_sem.at[i]) for i, s in enumerate(at)]
    writes = [pltpu.make_async_copy(buf.at[i], o_ref.at[:, s], out_sem.at[i]) for i, s in enumerate(at)]
    for c in reads:
        c.start()
    for r, w in zip(reads, writes):
        r.wait()
        w.start()
    for c in writes:
        c.wait()


def solution(mesh):
    def local(x, expert, slot, gate, w_gate, w_up, w_down):
        tokens, d = x.shape[2:]
        ff = w_gate.shape[2]
        top = expert.shape[3]
        chunks = d // 512
        slots = 5 * tokens * top // (4 * 8 * w_gate.shape[0])
        depth_in, depth_out = 3, 3
        anywhere = pl.BlockSpec(memory_space=pl.ANY)
        vmem = pl.BlockSpec(memory_space=pltpu.VMEM)
        y = pl.pallas_call(
            functools.partial(kernel, (d, ff, chunks, slots, depth_in, depth_out)),
            out_shape=jax.ShapeDtypeStruct((tokens, d), BF),
            in_specs=[anywhere, vmem, vmem, vmem, anywhere, anywhere, anywhere],
            out_specs=anywhere,
            scratch_shapes=[
                pltpu.VMEM((chunks, tokens, 512), BF),
                pltpu.VMEM((2, 320, tokens), BF),
                pltpu.VMEM((2 * tokens, 16 * 80), BF),
                pltpu.VMEM((2, chunks, 8, 80, 256), BF),
                pltpu.VMEM((2, chunks, 8, 80, 256), BF),
                pltpu.VMEM((chunks, 2, 8, 80, 256), BF),
                pltpu.VMEM((320, 512), BF),
                pltpu.VMEM((2, 320, ff), F32),
                pltpu.VMEM((320, ff), BF),
                pltpu.VMEM((depth_in, 512, ff), BF),
                pltpu.VMEM((depth_out, ff, 512), BF),
                pltpu.SemaphoreType.DMA((chunks,)),
                pltpu.SemaphoreType.DMA((depth_in,)),
                pltpu.SemaphoreType.DMA((depth_out,)),
                pltpu.SemaphoreType.DMA((2,)),
                pltpu.SemaphoreType.DMA((2, chunks)),
                pltpu.SemaphoreType.DMA((2,)),
                pltpu.SemaphoreType.DMA((2, chunks)),
                pltpu.SemaphoreType.DMA((chunks,)),
            ],
            compiler_params=pltpu.CompilerParams(collective_id=0, has_side_effects=True,
                                                 vmem_limit_bytes=67043328),
        )(x.reshape(tokens, d), expert.reshape(tokens, top).T, slot.reshape(tokens, top).T,
          gate.reshape(tokens, top).T,
          w_gate, w_up, w_down)
        y = pl.pallas_call(
            functools.partial(settle, chunks),
            out_shape=jax.ShapeDtypeStruct((tokens, d), BF),
            in_specs=[anywhere],
            out_specs=anywhere,
            scratch_shapes=[pltpu.VMEM((chunks, tokens, d // chunks), BF), pltpu.SemaphoreType.DMA((chunks,)),
                            pltpu.SemaphoreType.DMA((chunks,))],
            compiler_params=pltpu.CompilerParams(vmem_limit_bytes=60000000),
        )(y)
        return y.reshape(x.shape)

    tok = P("dp", "ep", None, None)
    wts = P("ep", None, None)
    return jax.shard_map(local, mesh=mesh, in_specs=(tok, tok, tok, tok, wts, wts, wts), out_specs=tok,
                         check_vma=False)
```

```python
import functools

import jax
import jax.numpy as jnp
from jax import lax
from jax.experimental import pallas as pl
from jax.experimental.pallas import tpu as pltpu
from jax.sharding import PartitionSpec as P

MESH = pl.DeviceIdType.MESH
BF = jnp.bfloat16
F32 = jnp.float32


def peer(me, r):
    x, y, c = me // 4, (me // 2) % 2, me % 2
    return ((x + r // 4) % 2) * 4 + ((y + (r // 2) % 2) % 2) * 2 + (c + r % 2) % 2


def block_of(o, r):
    a, b = slice(32 * r, 32 * r + 32), slice(256 + 8 * r, 264 + 8 * r)
    return jnp.concatenate([o[a, :256], o[b, :256], o[b, 256:], o[a, 256:]], axis=0).astype(BF)


def kernel(dims, x_ref, ex_ref, sl_ref, gt_ref, wg_ref, wu_ref, wd_ref, y_ref,
           to_slots, weigh, send, z_in, back, z, acc, h, w_in, w_out,
           x_sem, in_sem, out_sem, send_sem, z_sem, back_send_sem, back_sem):
    d, ff, chunks, slots, depth_in, depth_out = dims
    tokens = 256
    me = lax.axis_index("ep")

    def w_in_copy(e, k, m, slot):
        src = (wg_ref, wu_ref)[m]
        return pltpu.make_async_copy(src.at[e, pl.ds(k * 512, 512), :], w_in.at[slot], in_sem.at[slot])

    def w_out_copy(e, c, slot):
        return pltpu.make_async_copy(wd_ref.at[e, :, pl.ds(pl.multiple_of(c * 512, 512), 512)], w_out.at[slot],
                                     out_sem.at[slot])

    def columns(k):
        return pl.ds(pl.multiple_of(k * 512, 512), 512)

    def x_copy(k):
        return pltpu.make_async_copy(x_ref.at[:, columns(k)], y_ref.at[:, columns(k)], x_sem.at[k])

    barrier = pltpu.get_barrier_semaphore()
    for r in range(1, 8):
        pl.semaphore_signal(barrier, inc=1, device_id={"ep": peer(me, r)}, device_id_type=MESH)

    for k in range(chunks):
        x_copy(k).start()

    ex, sl = ex_ref[...], sl_ref[...]
    keep = sl < slots
    rel = jnp.bitwise_xor(ex // 2, me)
    half = ex % 2
    place = half * 320 + jnp.where(sl < 32, rel * 32 + sl, 256 + rel * 8 + sl - 32)
    place = jnp.where(keep, place, -1)
    p0, p1 = place[0:1, :], place[1:2, :]
    for e in range(2):
        row = lax.broadcasted_iota(jnp.int32, (320, tokens), 0) + 320 * e
        hit = jnp.where(row == p0, 1.0, jnp.where(row == p1, 1.0, 0.0))
        to_slots[e] = hit.astype(BF)

    pl.semaphore_wait(barrier, 7)

    def dispatch(i, _):
        e, k = i // chunks, i % chunks

        @pl.when(e == 0)
        def _():
            x_copy(k).wait()

        o = jnp.dot(to_slots[e], y_ref[:, columns(k)], preferred_element_type=F32)
        z_in[e, k, 0] = block_of(o, 0)
        for r in range(1, 8):
            send[e, k, r] = block_of(o, r)
        for r in (6, 2, 7, 3, 4, 5, 1):
            pltpu.make_async_remote_copy(
                src_ref=send.at[e, k, r], dst_ref=z_in.at[e, k, r], send_sem=send_sem.at[e], recv_sem=z_sem.at[e, k],
                device_id={"ep": peer(me, r)}, device_id_type=MESH).start()

        @pl.when(i == 2)
        def _():
            for j in range(depth_in):
                w_in_copy(0, j // 2, j % 2, j).start()

        return 0

    lax.fori_loop(0, 2 * chunks, dispatch, 0)

    for i in range(depth_out):
        w_out_copy(0, i, i).start()

    tiles = [(slice(0, 320), n, 512) for n in range(0, ff - 511, 512)]
    tiles += [(slice(m, m + 160), ff - 256, 256) for m in (0, 160)]

    def expert(e, _):
        def project(k, last):
            pltpu.make_async_copy(z_in.at[e, k, pl.ds(1, 7)], z_in.at[e, k, pl.ds(1, 7)], z_sem.at[e, k]).wait()
            for r in range(8):
                z[32 * r:32 * r + 32, 0:256] = z_in[e, k, r, 0:32, :]
                z[32 * r:32 * r + 32, 256:512] = z_in[e, k, r, 48:80, :]
            for r in range(0, 8, 2):
                a, b = z_in[e, k, r, 32:48, :].astype(F32), z_in[e, k, r + 1, 32:48, :].astype(F32)
                z[256 + 8 * r:272 + 8 * r, 0:256] = jnp.concatenate([a[:8], b[:8]], axis=0).astype(BF)
                z[256 + 8 * r:272 + 8 * r, 256:512] = jnp.concatenate([a[8:], b[8:]], axis=0).astype(BF)
            for m in range(2):
                i = (e * chunks + k) * 2 + m
                slot = i % depth_in
                w_in_copy(e, k, m, slot).wait()
                for rows, n, w in tiles:
                    at = slice(n, n + w)
                    part = jnp.dot(z[rows, :], w_in[slot, :, at], preferred_element_type=F32)
                    if not last:
                        acc[m, rows, at] = jnp.where(k == 0, 0.0, acc[m, rows, at]) + part
                    elif m == 0:
                        acc[0, rows, at] += part
                    else:
                        g, u = acc[0, rows, at], acc[1, rows, at] + part
                        h[rows, at] = (jax.nn.silu(g) * u).astype(BF)
                later = i + depth_in
                for mm in range(2):
                    @pl.when(jnp.logical_and(later < 4 * chunks, later % 2 == mm))
                    def _():
                        w_in_copy(later // (2 * chunks), (later // 2) % chunks, mm, slot).start()
            return 0

        lax.fori_loop(0, chunks - 1, lambda k, _: project(k, False), 0)
        project(chunks - 1, True)

        pltpu.make_async_copy(send.at[e, :, pl.ds(1, 7)], send.at[e, :, pl.ds(1, 7)], send_sem.at[e]).wait()

        def finish(c, _):
            j = e * chunks + c
            slot = j % depth_out
            w_out_copy(e, c, slot).wait()
            o = jnp.dot(h[...], w_out[slot], preferred_element_type=F32)
            back[c, e, 0] = block_of(o, 0)
            for r in range(1, 8):
                send[e, c, r] = block_of(o, r)
            later = j + depth_out

            @pl.when(later < 2 * chunks)
            def _():
                w_out_copy(later // chunks, later % chunks, slot).start()

            for r in (6, 2, 7, 3, 4, 5, 1):
                pltpu.make_async_remote_copy(
                    src_ref=send.at[e, c, r], dst_ref=back.at[c, e, r], send_sem=back_send_sem.at[e],
                    recv_sem=back_sem.at[e, c], device_id={"ep": peer(me, r)}, device_id_type=MESH).start()
            return 0

        lax.fori_loop(0, chunks, finish, 0)
        return 0

    lax.fori_loop(0, 2, expert, 0)

    base = (half * 8 + rel) * 80
    left = jnp.where(keep, base + sl, -1).astype(F32)
    right = jnp.where(keep, base + jnp.where(sl < 32, 48 + sl, 8 + sl), -1).astype(F32)
    gt = gt_ref[...]
    rows = jnp.zeros((128, tokens), F32)
    line = lax.broadcasted_iota(jnp.int32, (128, tokens), 0)
    for i, v in enumerate((left[0:1], left[1:2], right[0:1], right[1:2], gt[0:1], gt[1:2])):
        rows = jnp.where(line == i, v, rows)
    down = rows.T
    col = lax.broadcasted_iota(jnp.int32, (tokens, 16 * 80), 1)
    for s in range(2):
        a0, a1 = (down[:, 2 * s + j:2 * s + j + 1].astype(jnp.int32) for j in range(2))
        weight = jnp.where(col == a0, down[:, 4:5], jnp.where(col == a1, down[:, 5:6], 0.0))
        weigh[s * tokens:(s + 1) * tokens, :] = weight.astype(BF)

    def gather(c, _):
        for e in range(2):
            pltpu.make_async_copy(back.at[c, e, pl.ds(1, 7)], back.at[c, e, pl.ds(1, 7)], back_sem.at[e, c]).wait()
        o = jnp.dot(weigh[...], back[c].reshape(16 * 80, 256), preferred_element_type=F32)
        y_ref[:, pl.ds(pl.multiple_of(c * 512, 512), 256)] = o[:tokens].astype(BF)
        y_ref[:, pl.ds(pl.multiple_of(c * 512 + 256, 256), 256)] = o[tokens:].astype(BF)
        return 0

    lax.fori_loop(0, chunks, gather, 0)
    for e in range(2):
        pltpu.make_async_copy(send.at[e, :, pl.ds(1, 7)], send.at[e, :, pl.ds(1, 7)], back_send_sem.at[e]).wait()


def solution(mesh):
    def local(x, expert, slot, gate, w_gate, w_up, w_down):
        tokens, d = x.shape[2:]
        ff = w_gate.shape[2]
        top = expert.shape[3]
        chunks = d // 512
        slots = 5 * tokens * top // (4 * 8 * w_gate.shape[0])
        depth_in, depth_out = 3, 3
        anywhere = pl.BlockSpec(memory_space=pl.ANY)
        vmem = pl.BlockSpec(memory_space=pltpu.VMEM)
        y = pl.pallas_call(
            functools.partial(kernel, (d, ff, chunks, slots, depth_in, depth_out)),
            out_shape=pltpu.VMEM((tokens, d), BF),
            in_specs=[anywhere, vmem, vmem, vmem, anywhere, anywhere, anywhere],
            out_specs=vmem,
            scratch_shapes=[
                pltpu.VMEM((2, 320, tokens), BF),
                pltpu.VMEM((2 * tokens, 16 * 80), BF),
                pltpu.VMEM((2, chunks, 8, 80, 256), BF),
                pltpu.VMEM((2, chunks, 8, 80, 256), BF),
                pltpu.VMEM((chunks, 2, 8, 80, 256), BF),
                pltpu.VMEM((320, 512), BF),
                pltpu.VMEM((2, 320, ff), F32),
                pltpu.VMEM((320, ff), BF),
                pltpu.VMEM((depth_in, 512, ff), BF),
                pltpu.VMEM((depth_out, ff, 512), BF),
                pltpu.SemaphoreType.DMA((chunks,)),
                pltpu.SemaphoreType.DMA((depth_in,)),
                pltpu.SemaphoreType.DMA((depth_out,)),
                pltpu.SemaphoreType.DMA((2,)),
                pltpu.SemaphoreType.DMA((2, chunks)),
                pltpu.SemaphoreType.DMA((2,)),
                pltpu.SemaphoreType.DMA((2, chunks)),
            ],
            compiler_params=pltpu.CompilerParams(collective_id=0, has_side_effects=True,
                                                 vmem_limit_bytes=64500000),
        )(x.reshape(tokens, d), expert.reshape(tokens, top).T, slot.reshape(tokens, top).T,
          gate.reshape(tokens, top).T,
          w_gate, w_up, w_down)
        return y.reshape(x.shape)

    tok = P("dp", "ep", None, None)
    wts = P("ep", None, None)
    return jax.shard_map(local, mesh=mesh, in_specs=(tok, tok, tok, tok, wts, wts, wts), out_specs=tok,
                         check_vma=False)
```

```python
import functools

import jax
import jax.numpy as jnp
from jax import lax
from jax.experimental import pallas as pl
from jax.experimental.pallas import tpu as pltpu
from jax.sharding import PartitionSpec as P

MESH = pl.DeviceIdType.MESH
BF = jnp.bfloat16
F32 = jnp.float32


def peer(me, r):
    x, y, c = me // 4, (me // 2) % 2, me % 2
    return ((x + r // 4) % 2) * 4 + ((y + (r // 2) % 2) % 2) * 2 + (c + r % 2) % 2


def block_of(o, r):
    a, b = slice(32 * r, 32 * r + 32), slice(256 + 8 * r, 264 + 8 * r)
    return jnp.concatenate([o[a, :256], o[b, :256], o[b, 256:], o[a, 256:]], axis=0).astype(BF)


def kernel(dims, x_ref, ex_ref, sl_ref, gt_ref, wg_ref, wu_ref, wd_ref, y_ref,
           to_slots, weigh, send, z_in, back, z, acc, h, w_in, w_out,
           x_sem, in_sem, out_sem, send_sem, z_sem, back_send_sem, back_sem):
    d, ff, chunks, slots, depth_in, depth_out = dims
    tokens = 256
    me = lax.axis_index("ep")

    def w_in_copy(e, k, m, slot):
        src = (wg_ref, wu_ref)[m]
        return pltpu.make_async_copy(src.at[e, pl.ds(k * 512, 512), :], w_in.at[slot], in_sem.at[slot])

    def w_out_copy(e, c, slot):
        return pltpu.make_async_copy(wd_ref.at[e, :, pl.ds(pl.multiple_of(c * 512, 512), 512)], w_out.at[slot],
                                     out_sem.at[slot])

    def columns(k):
        return pl.ds(pl.multiple_of(k * 512, 512), 512)

    def x_copy(part):
        at = (pl.ds(0, 512), pl.ds(512, d - 512))[part]
        return pltpu.make_async_copy(x_ref.at[:, at], y_ref.at[:, at], x_sem.at[part])

    barrier = pltpu.get_barrier_semaphore()
    for r in range(1, 8):
        pl.semaphore_signal(barrier, inc=1, device_id={"ep": peer(me, r)}, device_id_type=MESH)

    for part in range(2):
        x_copy(part).start()

    ex, sl = ex_ref[...], sl_ref[...]
    keep = sl < slots
    rel = jnp.bitwise_xor(ex // 2, me)
    half = ex % 2
    place = half * 320 + jnp.where(sl < 32, rel * 32 + sl, 256 + rel * 8 + sl - 32)
    place = jnp.where(keep, place, -1)
    p0, p1 = place[0:1, :], place[1:2, :]
    def choose(e):
        row = lax.broadcasted_iota(jnp.int32, (320, tokens), 0) + 320 * e
        hit = jnp.where(row == p0, 1.0, jnp.where(row == p1, 1.0, 0.0))
        to_slots[e] = hit.astype(BF)

    def collect(e, k):
        o = jnp.dot(to_slots[e], y_ref[:, columns(k)], preferred_element_type=F32)
        z_in[e, k, 0] = block_of(o, 0)
        for r in range(1, 8):
            send[e, k, r] = block_of(o, r)

    def post(e, k):
        for r in (6, 2, 7, 3, 4, 5, 1):
            pltpu.make_async_remote_copy(
                src_ref=send.at[e, k, r], dst_ref=z_in.at[e, k, r], send_sem=send_sem.at[e], recv_sem=z_sem.at[e, k],
                device_id={"ep": peer(me, r)}, device_id_type=MESH).start()

    choose(0)
    x_copy(0).wait()
    collect(0, 0)
    pl.semaphore_wait(barrier, 7)
    post(0, 0)
    x_copy(1).wait()
    for i in range(depth_in):
        w_in_copy(0, i // 2, i % 2, i).start()

    def dispatch(i, _):
        collect(i // chunks, i % chunks)
        post(i // chunks, i % chunks)
        return 0

    lax.fori_loop(1, chunks, dispatch, 0)
    choose(1)
    lax.fori_loop(chunks, 2 * chunks, dispatch, 0)

    for i in range(depth_out):
        w_out_copy(0, i, i).start()

    tiles = [(slice(0, 320), n, 512) for n in range(0, ff - 511, 512)]
    tiles += [(slice(m, m + 160), ff - 256, 256) for m in (0, 160)]

    def expert(e, _):
        def project(k, last):
            pltpu.make_async_copy(z_in.at[e, k, pl.ds(1, 7)], z_in.at[e, k, pl.ds(1, 7)], z_sem.at[e, k]).wait()
            for r in range(8):
                z[32 * r:32 * r + 32, 0:256] = z_in[e, k, r, 0:32, :]
                z[32 * r:32 * r + 32, 256:512] = z_in[e, k, r, 48:80, :]
            for r in range(0, 8, 2):
                a, b = z_in[e, k, r, 32:48, :].astype(F32), z_in[e, k, r + 1, 32:48, :].astype(F32)
                z[256 + 8 * r:272 + 8 * r, 0:256] = jnp.concatenate([a[:8], b[:8]], axis=0).astype(BF)
                z[256 + 8 * r:272 + 8 * r, 256:512] = jnp.concatenate([a[8:], b[8:]], axis=0).astype(BF)
            for m in range(2):
                i = (e * chunks + k) * 2 + m
                slot = i % depth_in
                w_in_copy(e, k, m, slot).wait()
                for rows, n, w in tiles:
                    at = slice(n, n + w)
                    part = jnp.dot(z[rows, :], w_in[slot, :, at], preferred_element_type=F32)
                    if not last:
                        acc[m, rows, at] = jnp.where(k == 0, 0.0, acc[m, rows, at]) + part
                    elif m == 0:
                        acc[0, rows, at] += part
                    else:
                        g, u = acc[0, rows, at], acc[1, rows, at] + part
                        h[rows, at] = (jax.nn.silu(g) * u).astype(BF)
                later = i + depth_in
                for mm in range(2):
                    @pl.when(jnp.logical_and(later < 4 * chunks, later % 2 == mm))
                    def _():
                        w_in_copy(later // (2 * chunks), (later // 2) % chunks, mm, slot).start()
            return 0

        lax.fori_loop(0, chunks - 1, lambda k, _: project(k, False), 0)
        project(chunks - 1, True)

        pltpu.make_async_copy(send.at[e, :, pl.ds(1, 7)], send.at[e, :, pl.ds(1, 7)], send_sem.at[e]).wait()

        def finish(c, _):
            j = e * chunks + c
            slot = j % depth_out
            w_out_copy(e, c, slot).wait()
            o = jnp.dot(h[...], w_out[slot], preferred_element_type=F32)
            back[c, e, 0] = block_of(o, 0)
            for r in range(1, 8):
                send[e, c, r] = block_of(o, r)
            later = j + depth_out

            @pl.when(later < 2 * chunks)
            def _():
                w_out_copy(later // chunks, later % chunks, slot).start()

            for r in (6, 2, 7, 3, 4, 5, 1):
                pltpu.make_async_remote_copy(
                    src_ref=send.at[e, c, r], dst_ref=back.at[c, e, r], send_sem=back_send_sem.at[e],
                    recv_sem=back_sem.at[e * (1 + c)], device_id={"ep": peer(me, r)}, device_id_type=MESH).start()
            return 0

        lax.fori_loop(0, chunks, finish, 0)
        return 0

    lax.fori_loop(0, 2, expert, 0)

    base = (half * 8 + rel) * 80
    left = jnp.where(keep, base + sl, -1).astype(F32)
    right = jnp.where(keep, base + jnp.where(sl < 32, 48 + sl, 8 + sl), -1).astype(F32)
    gt = gt_ref[...]
    rows = jnp.zeros((128, tokens), F32)
    line = lax.broadcasted_iota(jnp.int32, (128, tokens), 0)
    for i, v in enumerate((left[0:1], left[1:2], right[0:1], right[1:2], gt[0:1], gt[1:2])):
        rows = jnp.where(line == i, v, rows)
    down = rows.T
    col = lax.broadcasted_iota(jnp.int32, (tokens, 16 * 80), 1)
    for s in range(2):
        a0, a1 = (down[:, 2 * s + j:2 * s + j + 1].astype(jnp.int32) for j in range(2))
        weight = jnp.where(col == a0, down[:, 4:5], jnp.where(col == a1, down[:, 5:6], 0.0))
        weigh[s * tokens:(s + 1) * tokens, :] = weight.astype(BF)

    pltpu.make_async_copy(back.at[:, 0, pl.ds(1, 7)], back.at[:, 0, pl.ds(1, 7)], back_sem.at[0]).wait()

    def share(c, e):
        o = jnp.dot(weigh[:, 640 * e:640 * (e + 1)], back[c, e].reshape(640, 256), preferred_element_type=F32)
        return o[:tokens], o[tokens:]

    def first(c, _):
        o = share(c, 0)
        for m in range(2):
            acc[m, 0:tokens, pl.ds(pl.multiple_of(c * 256, 256), 256)] = o[m]
        return 0

    def gather(c, _):
        pltpu.make_async_copy(back.at[c, 1, pl.ds(1, 7)], back.at[c, 1, pl.ds(1, 7)], back_sem.at[1 + c]).wait()
        o = share(c, 1)
        for m in range(2):
            y = acc[m, 0:tokens, pl.ds(pl.multiple_of(c * 256, 256), 256)] + o[m]
            y_ref[:, pl.ds(pl.multiple_of(c * 512 + 256 * m, 256), 256)] = y.astype(BF)
        return 0

    lax.fori_loop(0, chunks, first, 0)
    lax.fori_loop(0, chunks, gather, 0)
    for e in range(2):
        pltpu.make_async_copy(send.at[e, :, pl.ds(1, 7)], send.at[e, :, pl.ds(1, 7)], back_send_sem.at[e]).wait()


def solution(mesh):
    def local(x, expert, slot, gate, w_gate, w_up, w_down):
        tokens, d = x.shape[2:]
        ff = w_gate.shape[2]
        top = expert.shape[3]
        chunks = d // 512
        slots = 5 * tokens * top // (4 * 8 * w_gate.shape[0])
        depth_in, depth_out = 3, 3
        anywhere = pl.BlockSpec(memory_space=pl.ANY)
        vmem = pl.BlockSpec(memory_space=pltpu.VMEM)
        y = pl.pallas_call(
            functools.partial(kernel, (d, ff, chunks, slots, depth_in, depth_out)),
            out_shape=pltpu.VMEM((tokens, d), BF),
            in_specs=[anywhere, vmem, vmem, vmem, anywhere, anywhere, anywhere],
            out_specs=vmem,
            scratch_shapes=[
                pltpu.VMEM((2, 320, tokens), BF),
                pltpu.VMEM((2 * tokens, 16 * 80), BF),
                pltpu.VMEM((2, chunks, 8, 80, 256), BF),
                pltpu.VMEM((2, chunks, 8, 80, 256), BF),
                pltpu.VMEM((chunks, 2, 8, 80, 256), BF),
                pltpu.VMEM((320, 512), BF),
                pltpu.VMEM((2, 320, ff), F32),
                pltpu.VMEM((320, ff), BF),
                pltpu.VMEM((depth_in, 512, ff), BF),
                pltpu.VMEM((depth_out, ff, 512), BF),
                pltpu.SemaphoreType.DMA((2,)),
                pltpu.SemaphoreType.DMA((depth_in,)),
                pltpu.SemaphoreType.DMA((depth_out,)),
                pltpu.SemaphoreType.DMA((2,)),
                pltpu.SemaphoreType.DMA((2, chunks)),
                pltpu.SemaphoreType.DMA((2,)),
                pltpu.SemaphoreType.DMA((1 + chunks,)),
            ],
            compiler_params=pltpu.CompilerParams(collective_id=0, has_side_effects=True,
                                                 vmem_limit_bytes=64500000),
        )(x.reshape(tokens, d), expert.reshape(tokens, top).T, slot.reshape(tokens, top).T,
          gate.reshape(tokens, top).T,
          w_gate, w_up, w_down)
        return y.reshape(x.shape)

    tok = P("dp", "ep", None, None)
    wts = P("ep", None, None)
    return jax.shard_map(local, mesh=mesh, in_specs=(tok, tok, tok, tok, wts, wts, wts), out_specs=tok,
                         check_vma=False)
```

```python
import functools

import jax
import jax.numpy as jnp
from jax import lax
from jax.experimental import pallas as pl
from jax.experimental.pallas import tpu as pltpu
from jax.sharding import PartitionSpec as P

MESH = pl.DeviceIdType.MESH
BF = jnp.bfloat16
F32 = jnp.float32


def peer(me, r):
    x, y, c = me // 4, (me // 2) % 2, me % 2
    return ((x + r // 4) % 2) * 4 + ((y + (r // 2) % 2) % 2) * 2 + (c + r % 2) % 2


def block_of(o, r):
    a, b = slice(32 * r, 32 * r + 32), slice(256 + 8 * r, 264 + 8 * r)
    return jnp.concatenate([o[a, :256], o[b, :256], o[b, 256:], o[a, 256:]], axis=0).astype(BF)


def kernel(dims, x_ref, ex_hbm, sl_hbm, gt_hbm, wg_ref, wu_ref, wd_ref, y_ref,
           ex_ref, sl_ref, gt_ref, to_slots, weigh, send, z_in, back, z, acc, h, w_in, w_out,
           route_sem, x_sem, in_sem, out_sem, send_sem, z_sem, back_send_sem, back_sem):
    d, ff, chunks, slots, depth_in, depth_out = dims
    tokens = 256
    me = lax.axis_index("ep")

    def w_in_copy(e, k, m, slot):
        src = (wg_ref, wu_ref)[m]
        return pltpu.make_async_copy(src.at[e, pl.ds(k * 512, 512), :], w_in.at[slot], in_sem.at[slot])

    def w_out_copy(e, c, slot):
        return pltpu.make_async_copy(wd_ref.at[e, :, pl.ds(pl.multiple_of(c * 512, 512), 512)], w_out.at[slot],
                                     out_sem.at[slot])

    def columns(k):
        return pl.ds(pl.multiple_of(k * 512, 512), 512)

    def x_copy(part):
        at = (pl.ds(0, 512), pl.ds(512, d - 512))[part]
        return pltpu.make_async_copy(x_ref.at[:, at], y_ref.at[:, at], x_sem.at[part])

    barrier = pltpu.get_barrier_semaphore()
    for r in range(1, 8):
        pl.semaphore_signal(barrier, inc=1, device_id={"ep": peer(me, r)}, device_id_type=MESH)

    routes = [pltpu.make_async_copy(a, b, route_sem.at[i])
              for i, (a, b) in enumerate(((ex_hbm, ex_ref), (sl_hbm, sl_ref), (gt_hbm, gt_ref)))]
    for copy in routes:
        copy.start()
    for part in range(2):
        x_copy(part).start()
    for copy in routes:
        copy.wait()

    ex, sl = ex_ref[...], sl_ref[...]
    keep = sl < slots
    rel = jnp.bitwise_xor(ex // 2, me)
    half = ex % 2
    place = half * 320 + jnp.where(sl < 32, rel * 32 + sl, 256 + rel * 8 + sl - 32)
    place = jnp.where(keep, place, -1)
    p0, p1 = place[0:1, :], place[1:2, :]

    def choose(e):
        row = lax.broadcasted_iota(jnp.int32, (320, tokens), 0) + 320 * e
        hit = jnp.where(row == p0, 1.0, jnp.where(row == p1, 1.0, 0.0))
        to_slots[e] = hit.astype(BF)

    def collect(e, k):
        o = jnp.dot(to_slots[e], y_ref[:, columns(k)], preferred_element_type=F32)
        z_in[e, k, 0] = block_of(o, 0)
        for r in range(1, 8):
            send[e, k, r] = block_of(o, r)

    def post(e, k):
        for r in (6, 2, 7, 3, 4, 5, 1):
            pltpu.make_async_remote_copy(
                src_ref=send.at[e, k, r], dst_ref=z_in.at[e, k, r], send_sem=send_sem.at[e], recv_sem=z_sem.at[e, k],
                device_id={"ep": peer(me, r)}, device_id_type=MESH).start()

    choose(0)
    x_copy(0).wait()
    collect(0, 0)
    pl.semaphore_wait(barrier, 7)
    post(0, 0)
    x_copy(1).wait()
    for i in range(depth_in):
        w_in_copy(0, i // 2, i % 2, i).start()

    def dispatch(i, _):
        collect(i // chunks, i % chunks)
        post(i // chunks, i % chunks)
        return 0

    lax.fori_loop(1, chunks, dispatch, 0)
    choose(1)
    lax.fori_loop(chunks, 2 * chunks, dispatch, 0)

    for i in range(depth_out):
        w_out_copy(0, i, i).start()

    tiles = [(slice(0, 320), n, 512) for n in range(0, ff - 511, 512)]
    tiles += [(slice(m, m + 160), ff - 256, 256) for m in (0, 160)]

    def expert(e, _):
        def project(k, last):
            pltpu.make_async_copy(z_in.at[e, k, pl.ds(1, 7)], z_in.at[e, k, pl.ds(1, 7)], z_sem.at[e, k]).wait()
            for r in range(8):
                z[32 * r:32 * r + 32, 0:256] = z_in[e, k, r, 0:32, :]
                z[32 * r:32 * r + 32, 256:512] = z_in[e, k, r, 48:80, :]
            for r in range(0, 8, 2):
                a, b = z_in[e, k, r, 32:48, :].astype(F32), z_in[e, k, r + 1, 32:48, :].astype(F32)
                z[256 + 8 * r:272 + 8 * r, 0:256] = jnp.concatenate([a[:8], b[:8]], axis=0).astype(BF)
                z[256 + 8 * r:272 + 8 * r, 256:512] = jnp.concatenate([a[8:], b[8:]], axis=0).astype(BF)
            for m in range(2):
                i = (e * chunks + k) * 2 + m
                slot = i % depth_in
                w_in_copy(e, k, m, slot).wait()
                for rows, n, w in tiles:
                    at = slice(n, n + w)
                    part = jnp.dot(z[rows, :], w_in[slot, :, at], preferred_element_type=F32)
                    if not last:
                        acc[m, rows, at] = jnp.where(k == 0, 0.0, acc[m, rows, at]) + part
                    elif m == 0:
                        acc[0, rows, at] += part
                    else:
                        g, u = acc[0, rows, at], acc[1, rows, at] + part
                        h[rows, at] = (jax.nn.silu(g) * u).astype(BF)
                later = i + depth_in
                for mm in range(2):
                    @pl.when(jnp.logical_and(later < 4 * chunks, later % 2 == mm))
                    def _():
                        w_in_copy(later // (2 * chunks), (later // 2) % chunks, mm, slot).start()
            return 0

        lax.fori_loop(0, chunks - 1, lambda k, _: project(k, False), 0)
        project(chunks - 1, True)

        pltpu.make_async_copy(send.at[e, :, pl.ds(1, 7)], send.at[e, :, pl.ds(1, 7)], send_sem.at[e]).wait()

        def finish(c, _):
            j = e * chunks + c
            slot = j % depth_out
            w_out_copy(e, c, slot).wait()
            o = jnp.dot(h[...], w_out[slot], preferred_element_type=F32)
            back[c, e, 0] = block_of(o, 0)
            for r in range(1, 8):
                send[e, c, r] = block_of(o, r)
            later = j + depth_out

            @pl.when(later < 2 * chunks)
            def _():
                w_out_copy(later // chunks, later % chunks, slot).start()

            for r in (6, 2, 7, 3, 4, 5, 1):
                pltpu.make_async_remote_copy(
                    src_ref=send.at[e, c, r], dst_ref=back.at[c, e, r], send_sem=back_send_sem.at[e],
                    recv_sem=back_sem.at[e * (1 + c)], device_id={"ep": peer(me, r)}, device_id_type=MESH).start()
            return 0

        lax.fori_loop(0, chunks, finish, 0)
        return 0

    lax.fori_loop(0, 2, expert, 0)

    base = (half * 8 + rel) * 80
    left = jnp.where(keep, base + sl, -1).astype(F32)
    right = jnp.where(keep, base + jnp.where(sl < 32, 48 + sl, 8 + sl), -1).astype(F32)
    gt = gt_ref[...]
    rows = jnp.zeros((128, tokens), F32)
    line = lax.broadcasted_iota(jnp.int32, (128, tokens), 0)
    for i, v in enumerate((left[0:1], left[1:2], right[0:1], right[1:2], gt[0:1], gt[1:2])):
        rows = jnp.where(line == i, v, rows)
    down = rows.T
    col = lax.broadcasted_iota(jnp.int32, (tokens, 16 * 80), 1)
    for s in range(2):
        a0, a1 = (down[:, 2 * s + j:2 * s + j + 1].astype(jnp.int32) for j in range(2))
        weight = jnp.where(col == a0, down[:, 4:5], jnp.where(col == a1, down[:, 5:6], 0.0))
        weigh[s * tokens:(s + 1) * tokens, :] = weight.astype(BF)

    pltpu.make_async_copy(back.at[:, 0, pl.ds(1, 7)], back.at[:, 0, pl.ds(1, 7)], back_sem.at[0]).wait()

    def share(c, e):
        o = jnp.dot(weigh[:, 640 * e:640 * (e + 1)], back[c, e].reshape(640, 256), preferred_element_type=F32)
        return o[:tokens], o[tokens:]

    def first(c, _):
        o = share(c, 0)
        for m in range(2):
            acc[m, 0:tokens, pl.ds(pl.multiple_of(c * 256, 256), 256)] = o[m]
        return 0

    def gather(c, _):
        pltpu.make_async_copy(back.at[c, 1, pl.ds(1, 7)], back.at[c, 1, pl.ds(1, 7)], back_sem.at[1 + c]).wait()
        o = share(c, 1)
        for m in range(2):
            y = acc[m, 0:tokens, pl.ds(pl.multiple_of(c * 256, 256), 256)] + o[m]
            y_ref[:, pl.ds(pl.multiple_of(c * 512 + 256 * m, 256), 256)] = y.astype(BF)
        return 0

    lax.fori_loop(0, chunks, first, 0)
    lax.fori_loop(0, chunks, gather, 0)
    for e in range(2):
        pltpu.make_async_copy(send.at[e, :, pl.ds(1, 7)], send.at[e, :, pl.ds(1, 7)], back_send_sem.at[e]).wait()


def solution(mesh):
    def local(x, expert, slot, gate, w_gate, w_up, w_down):
        tokens, d = x.shape[2:]
        ff = w_gate.shape[2]
        top = expert.shape[3]
        chunks = d // 512
        slots = 5 * tokens * top // (4 * 8 * w_gate.shape[0])
        depth_in, depth_out = 3, 3
        anywhere = pl.BlockSpec(memory_space=pl.ANY)
        vmem = pl.BlockSpec(memory_space=pltpu.VMEM)
        y = pl.pallas_call(
            functools.partial(kernel, (d, ff, chunks, slots, depth_in, depth_out)),
            out_shape=pltpu.VMEM((tokens, d), BF),
            in_specs=[anywhere] * 7,
            out_specs=vmem,
            scratch_shapes=[
                pltpu.VMEM((top, tokens), jnp.int32),
                pltpu.VMEM((top, tokens), jnp.int32),
                pltpu.VMEM((top, tokens), F32),
                pltpu.VMEM((2, 320, tokens), BF),
                pltpu.VMEM((2 * tokens, 16 * 80), BF),
                pltpu.VMEM((2, chunks, 8, 80, 256), BF),
                pltpu.VMEM((2, chunks, 8, 80, 256), BF),
                pltpu.VMEM((chunks, 2, 8, 80, 256), BF),
                pltpu.VMEM((320, 512), BF),
                pltpu.VMEM((2, 320, ff), F32),
                pltpu.VMEM((320, ff), BF),
                pltpu.VMEM((depth_in, 512, ff), BF),
                pltpu.VMEM((depth_out, ff, 512), BF),
                pltpu.SemaphoreType.DMA((3,)),
                pltpu.SemaphoreType.DMA((2,)),
                pltpu.SemaphoreType.DMA((depth_in,)),
                pltpu.SemaphoreType.DMA((depth_out,)),
                pltpu.SemaphoreType.DMA((2,)),
                pltpu.SemaphoreType.DMA((2, chunks)),
                pltpu.SemaphoreType.DMA((2,)),
                pltpu.SemaphoreType.DMA((1 + chunks,)),
            ],
            compiler_params=pltpu.CompilerParams(collective_id=0, has_side_effects=True,
                                                 vmem_limit_bytes=64500000),
        )(x.reshape(tokens, d), expert.reshape(tokens, top).T, slot.reshape(tokens, top).T,
          gate.reshape(tokens, top).T,
          w_gate, w_up, w_down)
        return y.reshape(x.shape)

    tok = P("dp", "ep", None, None)
    wts = P("ep", None, None)
    return jax.shard_map(local, mesh=mesh, in_specs=(tok, tok, tok, tok, wts, wts, wts), out_specs=tok,
                         check_vma=False)
```

```python
import functools

import jax
import jax.numpy as jnp
from jax import lax
from jax.experimental import pallas as pl
from jax.experimental.pallas import tpu as pltpu
from jax.sharding import PartitionSpec as P

MESH = pl.DeviceIdType.MESH
BF = jnp.bfloat16
F32 = jnp.float32


def peer(me, r):
    x, y, c = me // 4, (me // 2) % 2, me % 2
    return ((x + r // 4) % 2) * 4 + ((y + (r // 2) % 2) % 2) * 2 + (c + r % 2) % 2


def block_of(o, r):
    a, b = slice(32 * r, 32 * r + 32), slice(256 + 8 * r, 264 + 8 * r)
    return jnp.concatenate([o[a, :256], o[b, :256], o[b, 256:], o[a, 256:]], axis=0).astype(BF)


def kernel(dims, x_ref, ex_hbm, sl_hbm, gt_hbm, wg_ref, wu_ref, wd_ref, y_ref,
           ex_ref, sl_ref, gt_ref, to_slots, weigh, send, z_in, back, z, acc, h, w_in, w_out,
           route_sem, x_sem, in_sem, out_sem, send_sem, z_sem, back_send_sem, back_sem):
    d, ff, chunks, slots, depth_in, depth_out = dims
    tokens = 256
    me = lax.axis_index("ep")

    def w_in_copy(e, k, m, slot):
        src = (wg_ref, wu_ref)[m]
        return pltpu.make_async_copy(src.at[e, pl.ds(k * 512, 512), :], w_in.at[slot], in_sem.at[slot])

    def w_out_copy(e, c, slot):
        return pltpu.make_async_copy(wd_ref.at[e, :, pl.ds(pl.multiple_of(c * 512, 512), 512)], w_out.at[slot],
                                     out_sem.at[slot])

    def columns(k):
        return pl.ds(pl.multiple_of(k * 512, 512), 512)

    def x_copy(part):
        at = (pl.ds(0, 512), pl.ds(512, d - 512))[part]
        return pltpu.make_async_copy(x_ref.at[:, at], y_ref.at[:, at], x_sem.at[part])

    turn = 2 * (me % 2)
    order = (6 - turn, 2, 7 - turn, 3, 4 + turn, 5 + turn, 1)

    barrier = pltpu.get_barrier_semaphore()
    for r in range(1, 8):
        pl.semaphore_signal(barrier, inc=1, device_id={"ep": peer(me, r)}, device_id_type=MESH)

    routes = [pltpu.make_async_copy(a, b, route_sem.at[i])
              for i, (a, b) in enumerate(((ex_hbm, ex_ref), (sl_hbm, sl_ref), (gt_hbm, gt_ref)))]
    for copy in routes:
        copy.start()
    for part in range(2):
        x_copy(part).start()
    for copy in routes:
        copy.wait()

    ex, sl = ex_ref[...], sl_ref[...]
    keep = sl < slots
    rel = jnp.bitwise_xor(ex // 2, me)
    half = ex % 2
    place = half * 320 + jnp.where(sl < 32, rel * 32 + sl, 256 + rel * 8 + sl - 32)
    place = jnp.where(keep, place, -1)
    p0, p1 = place[0:1, :], place[1:2, :]

    def choose(e):
        row = lax.broadcasted_iota(jnp.int32, (320, tokens), 0) + 320 * e
        hit = jnp.where(row == p0, 1.0, jnp.where(row == p1, 1.0, 0.0))
        to_slots[e] = hit.astype(BF)

    def collect(e, k):
        o = jnp.dot(to_slots[e], y_ref[:, columns(k)], preferred_element_type=F32)
        z_in[e, k, 0] = block_of(o, 0)
        for r in range(1, 8):
            send[e, k, r] = block_of(o, r)

    def post(e, k):
        for r in order:
            pltpu.make_async_remote_copy(
                src_ref=send.at[e, k, r], dst_ref=z_in.at[e, k, r], send_sem=send_sem.at[e], recv_sem=z_sem.at[e, k],
                device_id={"ep": peer(me, r)}, device_id_type=MESH).start()

    choose(0)
    x_copy(0).wait()
    collect(0, 0)
    pl.semaphore_wait(barrier, 7)
    post(0, 0)
    x_copy(1).wait()
    for i in range(depth_in):
        w_in_copy(0, i // 2, i % 2, i).start()

    def dispatch(i, _):
        collect(i // chunks, i % chunks)
        post(i // chunks, i % chunks)
        return 0

    lax.fori_loop(1, chunks, dispatch, 0)
    choose(1)
    lax.fori_loop(chunks, 2 * chunks, dispatch, 0)

    for i in range(depth_out):
        w_out_copy(0, i, i).start()

    tiles = [(slice(0, 320), n, 512) for n in range(0, ff - 511, 512)]
    tiles += [(slice(m, m + 160), ff - 256, 256) for m in (0, 160)]

    def expert(e, _):
        def project(k, last):
            pltpu.make_async_copy(z_in.at[e, k, pl.ds(1, 7)], z_in.at[e, k, pl.ds(1, 7)], z_sem.at[e, k]).wait()
            for r in range(8):
                z[32 * r:32 * r + 32, 0:256] = z_in[e, k, r, 0:32, :]
                z[32 * r:32 * r + 32, 256:512] = z_in[e, k, r, 48:80, :]
            for r in range(0, 8, 2):
                a, b = z_in[e, k, r, 32:48, :].astype(F32), z_in[e, k, r + 1, 32:48, :].astype(F32)
                z[256 + 8 * r:272 + 8 * r, 0:256] = jnp.concatenate([a[:8], b[:8]], axis=0).astype(BF)
                z[256 + 8 * r:272 + 8 * r, 256:512] = jnp.concatenate([a[8:], b[8:]], axis=0).astype(BF)
            for m in range(2):
                i = (e * chunks + k) * 2 + m
                slot = i % depth_in
                w_in_copy(e, k, m, slot).wait()
                for rows, n, w in tiles:
                    at = slice(n, n + w)
                    part = jnp.dot(z[rows, :], w_in[slot, :, at], preferred_element_type=F32)
                    if not last:
                        acc[m, rows, at] = jnp.where(k == 0, 0.0, acc[m, rows, at]) + part
                    elif m == 0:
                        acc[0, rows, at] += part
                    else:
                        g, u = acc[0, rows, at], acc[1, rows, at] + part
                        h[rows, at] = (jax.nn.silu(g) * u).astype(BF)
                later = i + depth_in
                for mm in range(2):
                    @pl.when(jnp.logical_and(later < 4 * chunks, later % 2 == mm))
                    def _():
                        w_in_copy(later // (2 * chunks), (later // 2) % chunks, mm, slot).start()
            return 0

        lax.fori_loop(0, chunks - 1, lambda k, _: project(k, False), 0)
        project(chunks - 1, True)

        pltpu.make_async_copy(send.at[e, :, pl.ds(1, 7)], send.at[e, :, pl.ds(1, 7)], send_sem.at[e]).wait()

        def finish(c, _):
            j = e * chunks + c
            slot = j % depth_out
            w_out_copy(e, c, slot).wait()
            o = jnp.dot(h[...], w_out[slot], preferred_element_type=F32)
            back[c, e, 0] = block_of(o, 0)
            for r in range(1, 8):
                send[e, c, r] = block_of(o, r)
            later = j + depth_out

            @pl.when(later < 2 * chunks)
            def _():
                w_out_copy(later // chunks, later % chunks, slot).start()

            for r in order:
                pltpu.make_async_remote_copy(
                    src_ref=send.at[e, c, r], dst_ref=back.at[c, e, r], send_sem=back_send_sem.at[e],
                    recv_sem=back_sem.at[e * (1 + c)], device_id={"ep": peer(me, r)}, device_id_type=MESH).start()
            return 0

        lax.fori_loop(0, chunks, finish, 0)
        return 0

    lax.fori_loop(0, 2, expert, 0)

    base = (half * 8 + rel) * 80
    left = jnp.where(keep, base + sl, -1).astype(F32)
    right = jnp.where(keep, base + jnp.where(sl < 32, 48 + sl, 8 + sl), -1).astype(F32)
    gt = gt_ref[...]
    rows = jnp.zeros((128, tokens), F32)
    line = lax.broadcasted_iota(jnp.int32, (128, tokens), 0)
    for i, v in enumerate((left[0:1], left[1:2], right[0:1], right[1:2], gt[0:1], gt[1:2])):
        rows = jnp.where(line == i, v, rows)
    down = rows.T
    col = lax.broadcasted_iota(jnp.int32, (tokens, 16 * 80), 1)
    for s in range(2):
        a0, a1 = (down[:, 2 * s + j:2 * s + j + 1].astype(jnp.int32) for j in range(2))
        weight = jnp.where(col == a0, down[:, 4:5], jnp.where(col == a1, down[:, 5:6], 0.0))
        weigh[s * tokens:(s + 1) * tokens, :] = weight.astype(BF)

    pltpu.make_async_copy(back.at[:, 0, pl.ds(1, 7)], back.at[:, 0, pl.ds(1, 7)], back_sem.at[0]).wait()

    def share(c, e):
        o = jnp.dot(weigh[:, 640 * e:640 * (e + 1)], back[c, e].reshape(640, 256), preferred_element_type=F32)
        return o[:tokens], o[tokens:]

    def first(c, _):
        o = share(c, 0)
        for m in range(2):
            acc[m, 0:tokens, pl.ds(pl.multiple_of(c * 256, 256), 256)] = o[m]
        return 0

    def gather(c, _):
        pltpu.make_async_copy(back.at[c, 1, pl.ds(1, 7)], back.at[c, 1, pl.ds(1, 7)], back_sem.at[1 + c]).wait()
        o = share(c, 1)
        for m in range(2):
            y = acc[m, 0:tokens, pl.ds(pl.multiple_of(c * 256, 256), 256)] + o[m]
            y_ref[:, pl.ds(pl.multiple_of(c * 512 + 256 * m, 256), 256)] = y.astype(BF)
        return 0

    lax.fori_loop(0, chunks, first, 0)
    lax.fori_loop(0, chunks, gather, 0)
    for e in range(2):
        pltpu.make_async_copy(send.at[e, :, pl.ds(1, 7)], send.at[e, :, pl.ds(1, 7)], back_send_sem.at[e]).wait()


def solution(mesh):
    def local(x, expert, slot, gate, w_gate, w_up, w_down):
        tokens, d = x.shape[2:]
        ff = w_gate.shape[2]
        top = expert.shape[3]
        chunks = d // 512
        slots = 5 * tokens * top // (4 * 8 * w_gate.shape[0])
        depth_in, depth_out = 3, 3
        anywhere = pl.BlockSpec(memory_space=pl.ANY)
        vmem = pl.BlockSpec(memory_space=pltpu.VMEM)
        y = pl.pallas_call(
            functools.partial(kernel, (d, ff, chunks, slots, depth_in, depth_out)),
            out_shape=pltpu.VMEM((tokens, d), BF),
            in_specs=[anywhere] * 7,
            out_specs=vmem,
            scratch_shapes=[
                pltpu.VMEM((top, tokens), jnp.int32),
                pltpu.VMEM((top, tokens), jnp.int32),
                pltpu.VMEM((top, tokens), F32),
                pltpu.VMEM((2, 320, tokens), BF),
                pltpu.VMEM((2 * tokens, 16 * 80), BF),
                pltpu.VMEM((2, chunks, 8, 80, 256), BF),
                pltpu.VMEM((2, chunks, 8, 80, 256), BF),
                pltpu.VMEM((chunks, 2, 8, 80, 256), BF),
                pltpu.VMEM((320, 512), BF),
                pltpu.VMEM((2, 320, ff), F32),
                pltpu.VMEM((320, ff), BF),
                pltpu.VMEM((depth_in, 512, ff), BF),
                pltpu.VMEM((depth_out, ff, 512), BF),
                pltpu.SemaphoreType.DMA((3,)),
                pltpu.SemaphoreType.DMA((2,)),
                pltpu.SemaphoreType.DMA((depth_in,)),
                pltpu.SemaphoreType.DMA((depth_out,)),
                pltpu.SemaphoreType.DMA((2,)),
                pltpu.SemaphoreType.DMA((2, chunks)),
                pltpu.SemaphoreType.DMA((2,)),
                pltpu.SemaphoreType.DMA((1 + chunks,)),
            ],
            compiler_params=pltpu.CompilerParams(collective_id=0, has_side_effects=True,
                                                 vmem_limit_bytes=64500000),
        )(x.reshape(tokens, d), expert.reshape(tokens, top).T, slot.reshape(tokens, top).T,
          gate.reshape(tokens, top).T,
          w_gate, w_up, w_down)
        return y.reshape(x.shape)

    tok = P("dp", "ep", None, None)
    wts = P("ep", None, None)
    return jax.shard_map(local, mesh=mesh, in_specs=(tok, tok, tok, tok, wts, wts, wts), out_specs=tok,
                         check_vma=False)
```

```python
import functools

import jax
import jax.numpy as jnp
from jax import lax
from jax.experimental import pallas as pl
from jax.experimental.pallas import tpu as pltpu
from jax.sharding import PartitionSpec as P

MESH = pl.DeviceIdType.MESH
BF = jnp.bfloat16
F32 = jnp.float32


def peer(me, r):
    x, y, c = me // 4, (me // 2) % 2, me % 2
    return ((x + r // 4) % 2) * 4 + ((y + (r // 2) % 2) % 2) * 2 + (c + r % 2) % 2


def block_of(o, r):
    a, b = slice(32 * r, 32 * r + 32), slice(256 + 8 * r, 264 + 8 * r)
    return jnp.concatenate([o[a, :256], o[b, :256], o[b, 256:], o[a, 256:]], axis=0).astype(BF)


def kernel(dims, x_ref, ex_hbm, sl_hbm, gt_hbm, wg_ref, wu_ref, wd_ref, y_ref,
           to_slots, weigh, send, z_in, back, z, acc, h, w_in, w_out, ex_ref, sl_ref, gt_ref,
           route_sem, x_sem, in_sem, out_sem, send_sem, z_sem, back_send_sem, back_sem):
    d, ff, chunks, slots, depth_in, depth_out = dims
    tokens = 256
    me = lax.axis_index("ep")

    def w_in_copy(e, k, m, slot):
        src = (wg_ref, wu_ref)[m]
        return pltpu.make_async_copy(src.at[e, pl.ds(k * 512, 512), :], w_in.at[slot], in_sem.at[slot])

    def w_out_copy(e, c, slot):
        return pltpu.make_async_copy(wd_ref.at[e, :, pl.ds(pl.multiple_of(c * 512, 512), 512)], w_out.at[slot],
                                     out_sem.at[slot])

    def columns(k):
        return pl.ds(pl.multiple_of(k * 512, 512), 512)

    def x_copy(part):
        at = (pl.ds(0, 512), pl.ds(512, d - 512))[part]
        return pltpu.make_async_copy(x_ref.at[:, at], y_ref.at[:, at], x_sem.at[part])

    barrier = pltpu.get_barrier_semaphore()
    for r in range(1, 8):
        pl.semaphore_signal(barrier, inc=1, device_id={"ep": peer(me, r)}, device_id_type=MESH)

    routes = [pltpu.make_async_copy(a, b, route_sem.at[i])
              for i, (a, b) in enumerate(((ex_hbm, ex_ref), (sl_hbm, sl_ref), (gt_hbm, gt_ref)))]
    for copy in routes:
        copy.start()
    for part in range(2):
        x_copy(part).start()
    for copy in routes:
        copy.wait()

    ex, sl = ex_ref[...], sl_ref[...]
    keep = sl < slots
    rel = jnp.bitwise_xor(ex // 2, me)
    half = ex % 2
    place = half * 320 + jnp.where(sl < 32, rel * 32 + sl, 256 + rel * 8 + sl - 32)
    place = jnp.where(keep, place, -1)
    p0, p1 = place[0:1, :], place[1:2, :]

    def choose(e):
        row = lax.broadcasted_iota(jnp.int32, (320, tokens), 0) + 320 * e
        hit = jnp.where(row == p0, 1.0, jnp.where(row == p1, 1.0, 0.0))
        to_slots[e] = hit.astype(BF)

    def collect(e, k):
        o = jnp.dot(to_slots[e], y_ref[:, columns(k)], preferred_element_type=F32)
        z_in[e, k, 0] = block_of(o, 0)
        for r in range(1, 8):
            send[e, k, r] = block_of(o, r)

    def post(e, k):
        for r in (6, 2, 7, 3, 4, 5, 1):
            pltpu.make_async_remote_copy(
                src_ref=send.at[e, k, r], dst_ref=z_in.at[e, k, r], send_sem=send_sem.at[e], recv_sem=z_sem.at[e, k],
                device_id={"ep": peer(me, r)}, device_id_type=MESH).start()

    choose(0)
    x_copy(0).wait()
    collect(0, 0)
    pl.semaphore_wait(barrier, 7)
    post(0, 0)
    x_copy(1).wait()
    for i in range(depth_in):
        w_in_copy(0, i // 2, i % 2, i).start()

    def dispatch(i, _):
        collect(i // chunks, i % chunks)
        post(i // chunks, i % chunks)
        return 0

    lax.fori_loop(1, chunks, dispatch, 0)
    choose(1)
    lax.fori_loop(chunks, 2 * chunks, dispatch, 0)

    for i in range(depth_out):
        w_out_copy(0, i, i).start()

    tiles = [(slice(0, 320), n, 512) for n in range(0, ff - 511, 512)]
    tiles += [(slice(m, m + 160), ff - 256, 256) for m in (0, 160)]

    def expert(e, _):
        def project(k, last):
            pltpu.make_async_copy(z_in.at[e, k, pl.ds(1, 7)], z_in.at[e, k, pl.ds(1, 7)], z_sem.at[e, k]).wait()
            for r in range(8):
                z[32 * r:32 * r + 32, 0:256] = z_in[e, k, r, 0:32, :]
                z[32 * r:32 * r + 32, 256:512] = z_in[e, k, r, 48:80, :]
            for r in range(0, 8, 2):
                a, b = z_in[e, k, r, 32:48, :].astype(F32), z_in[e, k, r + 1, 32:48, :].astype(F32)
                z[256 + 8 * r:272 + 8 * r, 0:256] = jnp.concatenate([a[:8], b[:8]], axis=0).astype(BF)
                z[256 + 8 * r:272 + 8 * r, 256:512] = jnp.concatenate([a[8:], b[8:]], axis=0).astype(BF)
            for m in range(2):
                i = (e * chunks + k) * 2 + m
                slot = i % depth_in
                w_in_copy(e, k, m, slot).wait()
                for rows, n, w in tiles:
                    at = slice(n, n + w)
                    part = jnp.dot(z[rows, :], w_in[slot, :, at], preferred_element_type=F32)
                    if not last:
                        acc[m, rows, at] = jnp.where(k == 0, 0.0, acc[m, rows, at]) + part
                    elif m == 0:
                        acc[0, rows, at] += part
                    else:
                        g, u = acc[0, rows, at], acc[1, rows, at] + part
                        h[rows, at] = (jax.nn.silu(g) * u).astype(BF)
                later = i + depth_in
                for mm in range(2):
                    @pl.when(jnp.logical_and(later < 4 * chunks, later % 2 == mm))
                    def _():
                        w_in_copy(later // (2 * chunks), (later // 2) % chunks, mm, slot).start()
            return 0

        lax.fori_loop(0, chunks - 1, lambda k, _: project(k, False), 0)
        project(chunks - 1, True)

        pltpu.make_async_copy(send.at[e, :, pl.ds(1, 7)], send.at[e, :, pl.ds(1, 7)], send_sem.at[e]).wait()

        def finish(c, _):
            j = e * chunks + c
            slot = j % depth_out
            w_out_copy(e, c, slot).wait()
            o = jnp.dot(h[...], w_out[slot], preferred_element_type=F32)
            back[c, e, 0] = block_of(o, 0)
            for r in range(1, 8):
                send[e, c, r] = block_of(o, r)
            later = j + depth_out

            @pl.when(later < 2 * chunks)
            def _():
                w_out_copy(later // chunks, later % chunks, slot).start()

            for r in (6, 2, 7, 3, 4, 5, 1):
                pltpu.make_async_remote_copy(
                    src_ref=send.at[e, c, r], dst_ref=back.at[c, e, r], send_sem=back_send_sem.at[e],
                    recv_sem=back_sem.at[e * (1 + c)], device_id={"ep": peer(me, r)}, device_id_type=MESH).start()
            return 0

        lax.fori_loop(0, chunks, finish, 0)
        return 0

    lax.fori_loop(0, 2, expert, 0)

    base = (half * 8 + rel) * 80
    left = jnp.where(keep, base + sl, -1).astype(F32)
    right = jnp.where(keep, base + jnp.where(sl < 32, 48 + sl, 8 + sl), -1).astype(F32)
    gt = gt_ref[...]
    rows = jnp.zeros((128, tokens), F32)
    line = lax.broadcasted_iota(jnp.int32, (128, tokens), 0)
    for i, v in enumerate((left[0:1], left[1:2], right[0:1], right[1:2], gt[0:1], gt[1:2])):
        rows = jnp.where(line == i, v, rows)
    down = rows.T
    col = lax.broadcasted_iota(jnp.int32, (tokens, 16 * 80), 1)
    for s in range(2):
        a0, a1 = (down[:, 2 * s + j:2 * s + j + 1].astype(jnp.int32) for j in range(2))
        weight = jnp.where(col == a0, down[:, 4:5], jnp.where(col == a1, down[:, 5:6], 0.0))
        weigh[s * tokens:(s + 1) * tokens, :] = weight.astype(BF)

    pltpu.make_async_copy(back.at[:, 0, pl.ds(1, 7)], back.at[:, 0, pl.ds(1, 7)], back_sem.at[0]).wait()

    def share(c, e):
        o = jnp.dot(weigh[:, 640 * e:640 * (e + 1)], back[c, e].reshape(640, 256), preferred_element_type=F32)
        return o[:tokens], o[tokens:]

    def first(c, _):
        o = share(c, 0)
        for m in range(2):
            acc[m, 0:tokens, pl.ds(pl.multiple_of(c * 256, 256), 256)] = o[m]
        return 0

    def gather(c, _):
        pltpu.make_async_copy(back.at[c, 1, pl.ds(1, 7)], back.at[c, 1, pl.ds(1, 7)], back_sem.at[1 + c]).wait()
        o = share(c, 1)
        for m in range(2):
            y = acc[m, 0:tokens, pl.ds(pl.multiple_of(c * 256, 256), 256)] + o[m]
            y_ref[:, pl.ds(pl.multiple_of(c * 512 + 256 * m, 256), 256)] = y.astype(BF)
        return 0

    lax.fori_loop(0, chunks, first, 0)
    lax.fori_loop(0, chunks, gather, 0)
    for e in range(2):
        pltpu.make_async_copy(send.at[e, :, pl.ds(1, 7)], send.at[e, :, pl.ds(1, 7)], back_send_sem.at[e]).wait()


def solution(mesh):
    def local(x, expert, slot, gate, w_gate, w_up, w_down):
        tokens, d = x.shape[2:]
        ff = w_gate.shape[2]
        top = expert.shape[3]
        chunks = d // 512
        slots = 5 * tokens * top // (4 * 8 * w_gate.shape[0])
        depth_in, depth_out = 3, 3
        anywhere = pl.BlockSpec(memory_space=pl.ANY)
        vmem = pl.BlockSpec(memory_space=pltpu.VMEM)
        y = pl.pallas_call(
            functools.partial(kernel, (d, ff, chunks, slots, depth_in, depth_out)),
            out_shape=pltpu.VMEM((tokens, d), BF),
            in_specs=[anywhere] * 7,
            out_specs=vmem,
            scratch_shapes=[
                pltpu.VMEM((2, 320, tokens), BF),
                pltpu.VMEM((2 * tokens, 16 * 80), BF),
                pltpu.VMEM((2, chunks, 8, 80, 256), BF),
                pltpu.VMEM((2, chunks, 8, 80, 256), BF),
                pltpu.VMEM((chunks, 2, 8, 80, 256), BF),
                pltpu.VMEM((320, 512), BF),
                pltpu.VMEM((2, 320, ff), F32),
                pltpu.VMEM((320, ff), BF),
                pltpu.VMEM((depth_in, 512, ff), BF),
                pltpu.VMEM((depth_out, ff, 512), BF),
                pltpu.VMEM((top, tokens), jnp.int32),
                pltpu.VMEM((top, tokens), jnp.int32),
                pltpu.VMEM((top, tokens), F32),
                pltpu.SemaphoreType.DMA((3,)),
                pltpu.SemaphoreType.DMA((2,)),
                pltpu.SemaphoreType.DMA((depth_in,)),
                pltpu.SemaphoreType.DMA((depth_out,)),
                pltpu.SemaphoreType.DMA((2,)),
                pltpu.SemaphoreType.DMA((2, chunks)),
                pltpu.SemaphoreType.DMA((2,)),
                pltpu.SemaphoreType.DMA((1 + chunks,)),
            ],
            compiler_params=pltpu.CompilerParams(collective_id=0, has_side_effects=True,
                                                 vmem_limit_bytes=64500000),
        )(x.reshape(tokens, d), expert.reshape(tokens, top).T, slot.reshape(tokens, top).T,
          gate.reshape(tokens, top).T,
          w_gate, w_up, w_down)
        return y.reshape(x.shape)

    tok = P("dp", "ep", None, None)
    wts = P("ep", None, None)
    return jax.shard_map(local, mesh=mesh, in_specs=(tok, tok, tok, tok, wts, wts, wts), out_specs=tok,
                         check_vma=False)
```

```python
import functools

import jax
import jax.numpy as jnp
from jax import lax
from jax.experimental import pallas as pl
from jax.experimental.pallas import tpu as pltpu
from jax.sharding import PartitionSpec as P

MESH = pl.DeviceIdType.MESH
BF = jnp.bfloat16
F32 = jnp.float32


def peer(me, r):
    x, y, c = me // 4, (me // 2) % 2, me % 2
    return ((x + r // 4) % 2) * 4 + ((y + (r // 2) % 2) % 2) * 2 + (c + r % 2) % 2


def block_of(o, r):
    a, b = slice(32 * r, 32 * r + 32), slice(256 + 8 * r, 264 + 8 * r)
    return jnp.concatenate([o[a, :256], o[b, :256], o[b, 256:], o[a, 256:]], axis=0).astype(BF)


def kernel(dims, x_ref, ex_hbm, sl_hbm, gt_hbm, wg_ref, wu_ref, wd_ref, y_ref,
           send, z_in, back, z, acc, h, w_in, w_out, to_slots, weigh, ex_ref, sl_ref, gt_ref,
           route_sem, x_sem, in_sem, out_sem, send_sem, z_sem, back_send_sem, back_sem):
    d, ff, chunks, slots, depth_in, depth_out = dims
    tokens = 256
    me = lax.axis_index("ep")

    def w_in_copy(e, k, m, slot):
        src = (wg_ref, wu_ref)[m]
        return pltpu.make_async_copy(src.at[e, pl.ds(k * 512, 512), :], w_in.at[slot], in_sem.at[slot])

    def w_out_copy(e, c, slot):
        return pltpu.make_async_copy(wd_ref.at[e, :, pl.ds(pl.multiple_of(c * 512, 512), 512)], w_out.at[slot],
                                     out_sem.at[slot])

    def columns(k):
        return pl.ds(pl.multiple_of(k * 512, 512), 512)

    def x_copy(part):
        at = (pl.ds(0, 512), pl.ds(512, d - 512))[part]
        return pltpu.make_async_copy(x_ref.at[:, at], y_ref.at[:, at], x_sem.at[part])

    barrier = pltpu.get_barrier_semaphore()
    for r in range(1, 8):
        pl.semaphore_signal(barrier, inc=1, device_id={"ep": peer(me, r)}, device_id_type=MESH)

    routes = [pltpu.make_async_copy(a, b, route_sem.at[i])
              for i, (a, b) in enumerate(((ex_hbm, ex_ref), (sl_hbm, sl_ref), (gt_hbm, gt_ref)))]
    for copy in routes:
        copy.start()
    for part in range(2):
        x_copy(part).start()
    for copy in routes:
        copy.wait()

    ex, sl = ex_ref[...], sl_ref[...]
    keep = sl < slots
    rel = jnp.bitwise_xor(ex // 2, me)
    half = ex % 2
    place = half * 320 + jnp.where(sl < 32, rel * 32 + sl, 256 + rel * 8 + sl - 32)
    place = jnp.where(keep, place, -1)
    p0, p1 = place[0:1, :], place[1:2, :]

    def choose(e):
        row = lax.broadcasted_iota(jnp.int32, (320, tokens), 0) + 320 * e
        hit = jnp.where(row == p0, 1.0, jnp.where(row == p1, 1.0, 0.0))
        to_slots[e] = hit.astype(BF)

    def collect(e, k):
        o = jnp.dot(to_slots[e], y_ref[:, columns(k)], preferred_element_type=F32)
        z_in[e, k, 0] = block_of(o, 0)
        for r in range(1, 8):
            send[e, k, r] = block_of(o, r)

    def post(e, k):
        for r in (6, 2, 7, 3, 4, 5, 1):
            pltpu.make_async_remote_copy(
                src_ref=send.at[e, k, r], dst_ref=z_in.at[e, k, r], send_sem=send_sem.at[e], recv_sem=z_sem.at[e, k],
                device_id={"ep": peer(me, r)}, device_id_type=MESH).start()

    choose(0)
    x_copy(0).wait()
    collect(0, 0)
    pl.semaphore_wait(barrier, 7)
    post(0, 0)
    x_copy(1).wait()
    for i in range(depth_in):
        w_in_copy(0, i // 2, i % 2, i).start()

    def dispatch(i, _):
        collect(i // chunks, i % chunks)
        post(i // chunks, i % chunks)
        return 0

    lax.fori_loop(1, chunks, dispatch, 0)
    choose(1)
    lax.fori_loop(chunks, 2 * chunks, dispatch, 0)

    for i in range(depth_out):
        w_out_copy(0, i, i).start()

    tiles = [(slice(0, 320), n, 512) for n in range(0, ff - 511, 512)]
    tiles += [(slice(m, m + 160), ff - 256, 256) for m in (0, 160)]

    def expert(e, _):
        def project(k, last):
            pltpu.make_async_copy(z_in.at[e, k, pl.ds(1, 7)], z_in.at[e, k, pl.ds(1, 7)], z_sem.at[e, k]).wait()
            for r in range(8):
                z[32 * r:32 * r + 32, 0:256] = z_in[e, k, r, 0:32, :]
                z[32 * r:32 * r + 32, 256:512] = z_in[e, k, r, 48:80, :]
            for r in range(0, 8, 2):
                a, b = z_in[e, k, r, 32:48, :].astype(F32), z_in[e, k, r + 1, 32:48, :].astype(F32)
                z[256 + 8 * r:272 + 8 * r, 0:256] = jnp.concatenate([a[:8], b[:8]], axis=0).astype(BF)
                z[256 + 8 * r:272 + 8 * r, 256:512] = jnp.concatenate([a[8:], b[8:]], axis=0).astype(BF)
            for m in range(2):
                i = (e * chunks + k) * 2 + m
                slot = i % depth_in
                w_in_copy(e, k, m, slot).wait()
                for rows, n, w in tiles:
                    at = slice(n, n + w)
                    part = jnp.dot(z[rows, :], w_in[slot, :, at], preferred_element_type=F32)
                    if not last:
                        acc[m, rows, at] = jnp.where(k == 0, 0.0, acc[m, rows, at]) + part
                    elif m == 0:
                        acc[0, rows, at] += part
                    else:
                        g, u = acc[0, rows, at], acc[1, rows, at] + part
                        h[rows, at] = (jax.nn.silu(g) * u).astype(BF)
                later = i + depth_in
                for mm in range(2):
                    @pl.when(jnp.logical_and(later < 4 * chunks, later % 2 == mm))
                    def _():
                        w_in_copy(later // (2 * chunks), (later // 2) % chunks, mm, slot).start()
            return 0

        lax.fori_loop(0, chunks - 1, lambda k, _: project(k, False), 0)
        project(chunks - 1, True)

        pltpu.make_async_copy(send.at[e, :, pl.ds(1, 7)], send.at[e, :, pl.ds(1, 7)], send_sem.at[e]).wait()

        def finish(c, _):
            j = e * chunks + c
            slot = j % depth_out
            w_out_copy(e, c, slot).wait()
            o = jnp.dot(h[...], w_out[slot], preferred_element_type=F32)
            back[c, e, 0] = block_of(o, 0)
            for r in range(1, 8):
                send[e, c, r] = block_of(o, r)
            later = j + depth_out

            @pl.when(later < 2 * chunks)
            def _():
                w_out_copy(later // chunks, later % chunks, slot).start()

            for r in (6, 2, 7, 3, 4, 5, 1):
                pltpu.make_async_remote_copy(
                    src_ref=send.at[e, c, r], dst_ref=back.at[c, e, r], send_sem=back_send_sem.at[e],
                    recv_sem=back_sem.at[e * (1 + c)], device_id={"ep": peer(me, r)}, device_id_type=MESH).start()
            return 0

        lax.fori_loop(0, chunks, finish, 0)
        return 0

    lax.fori_loop(0, 2, expert, 0)

    base = (half * 8 + rel) * 80
    left = jnp.where(keep, base + sl, -1).astype(F32)
    right = jnp.where(keep, base + jnp.where(sl < 32, 48 + sl, 8 + sl), -1).astype(F32)
    gt = gt_ref[...]
    rows = jnp.zeros((128, tokens), F32)
    line = lax.broadcasted_iota(jnp.int32, (128, tokens), 0)
    for i, v in enumerate((left[0:1], left[1:2], right[0:1], right[1:2], gt[0:1], gt[1:2])):
        rows = jnp.where(line == i, v, rows)
    down = rows.T
    col = lax.broadcasted_iota(jnp.int32, (tokens, 16 * 80), 1)
    for s in range(2):
        a0, a1 = (down[:, 2 * s + j:2 * s + j + 1].astype(jnp.int32) for j in range(2))
        weight = jnp.where(col == a0, down[:, 4:5], jnp.where(col == a1, down[:, 5:6], 0.0))
        weigh[s * tokens:(s + 1) * tokens, :] = weight.astype(BF)

    pltpu.make_async_copy(back.at[:, 0, pl.ds(1, 7)], back.at[:, 0, pl.ds(1, 7)], back_sem.at[0]).wait()

    def share(c, e):
        o = jnp.dot(weigh[:, 640 * e:640 * (e + 1)], back[c, e].reshape(640, 256), preferred_element_type=F32)
        return o[:tokens], o[tokens:]

    def first(c, _):
        o = share(c, 0)
        for m in range(2):
            acc[m, 0:tokens, pl.ds(pl.multiple_of(c * 256, 256), 256)] = o[m]
        return 0

    def gather(c, _):
        pltpu.make_async_copy(back.at[c, 1, pl.ds(1, 7)], back.at[c, 1, pl.ds(1, 7)], back_sem.at[1 + c]).wait()
        o = share(c, 1)
        for m in range(2):
            y = acc[m, 0:tokens, pl.ds(pl.multiple_of(c * 256, 256), 256)] + o[m]
            y_ref[:, pl.ds(pl.multiple_of(c * 512 + 256 * m, 256), 256)] = y.astype(BF)
        return 0

    lax.fori_loop(0, chunks, first, 0)
    lax.fori_loop(0, chunks, gather, 0)
    for e in range(2):
        pltpu.make_async_copy(send.at[e, :, pl.ds(1, 7)], send.at[e, :, pl.ds(1, 7)], back_send_sem.at[e]).wait()


def solution(mesh):
    def local(x, expert, slot, gate, w_gate, w_up, w_down):
        tokens, d = x.shape[2:]
        ff = w_gate.shape[2]
        top = expert.shape[3]
        chunks = d // 512
        slots = 5 * tokens * top // (4 * 8 * w_gate.shape[0])
        depth_in, depth_out = 3, 3
        anywhere = pl.BlockSpec(memory_space=pl.ANY)
        vmem = pl.BlockSpec(memory_space=pltpu.VMEM)
        y = pl.pallas_call(
            functools.partial(kernel, (d, ff, chunks, slots, depth_in, depth_out)),
            out_shape=pltpu.VMEM((tokens, d), BF),
            in_specs=[anywhere] * 7,
            out_specs=vmem,
            scratch_shapes=[
                pltpu.VMEM((2, chunks, 8, 80, 256), BF),
                pltpu.VMEM((2, chunks, 8, 80, 256), BF),
                pltpu.VMEM((chunks, 2, 8, 80, 256), BF),
                pltpu.VMEM((320, 512), BF),
                pltpu.VMEM((2, 320, ff), F32),
                pltpu.VMEM((320, ff), BF),
                pltpu.VMEM((depth_in, 512, ff), BF),
                pltpu.VMEM((depth_out, ff, 512), BF),
                pltpu.VMEM((2, 320, tokens), BF),
                pltpu.VMEM((2 * tokens, 16 * 80), BF),
                pltpu.VMEM((top, tokens), jnp.int32),
                pltpu.VMEM((top, tokens), jnp.int32),
                pltpu.VMEM((top, tokens), F32),
                pltpu.SemaphoreType.DMA((3,)),
                pltpu.SemaphoreType.DMA((2,)),
                pltpu.SemaphoreType.DMA((depth_in,)),
                pltpu.SemaphoreType.DMA((depth_out,)),
                pltpu.SemaphoreType.DMA((2,)),
                pltpu.SemaphoreType.DMA((2, chunks)),
                pltpu.SemaphoreType.DMA((2,)),
                pltpu.SemaphoreType.DMA((1 + chunks,)),
            ],
            compiler_params=pltpu.CompilerParams(collective_id=0, has_side_effects=True,
                                                 vmem_limit_bytes=64500000),
        )(x.reshape(tokens, d), expert.reshape(tokens, top).T, slot.reshape(tokens, top).T,
          gate.reshape(tokens, top).T,
          w_gate, w_up, w_down)
        return y.reshape(x.shape)

    tok = P("dp", "ep", None, None)
    wts = P("ep", None, None)
    return jax.shard_map(local, mesh=mesh, in_specs=(tok, tok, tok, tok, wts, wts, wts), out_specs=tok,
                         check_vma=False)
```
